128 devices in a mesh: tok: 16 (over z_lo, y, core), blk: 8 (over x, z_hi).
Axes of the slice: x: 4, y: 4, z: 4 (z_hi: 2, z_lo: 2; z = z_hi * 2 + z_lo), core: 2. Of those that a mesh axis runs over, the one named last changes fastest.
Arguments:
- activations: bfloat16 [8192, 4096], P('tok', 'blk'), may hold values from -52 to 52, as said below
- out_grads: bfloat16 [8192, 4096], P('tok', 'blk'), may hold values from -52 to 52, as said below
Outputs:
- act_inverse: float32 [4096, 4096], P(('tok', 'blk'))
- grad_inverse: float32 [4096, 4096], P(('tok', 'blk'))
The draws below stay inside these ranges and needn't reach their ends.
Inputs may be any that keep to these rules, and one draw needn't show every extreme that they name: `activations`: real entries. `out_grads`: real entries.
All inputs are finite; a program needn't handle non-finite values.
Results may differ from the reference program's by a relative error of at most 0.02.
Values may be sent and summed in bfloat16 or wider, within the bound.
No kernel may reach another device: no remote copies, remote signals or barrier semaphores. Data moves between devices by JAX's collectives and lax.ppermute only.
A program may use at most 64 MiB of HBM per device.

```python
import jax
import jax.numpy as jnp
from jax import lax

D = 4096
TOK_DEV = 512
TOKENS = 8192
N_TOK = 16


def scaled_draw(key):
    row_key, col_key, value_key = jax.random.split(key, 3)
    positions = jnp.arange(TOKENS, dtype=jnp.float32) / TOKENS
    values = jax.random.truncated_normal(value_key, -5.0, 5.0, (TOKENS, D), jnp.float32)
    row_scale = jnp.exp(jax.random.uniform(row_key, (TOKENS, 1), jnp.float32, 0.0, jnp.log(3.0)))
    ramp = jnp.exp(positions * 0.5 * jnp.log(3.0))
    col_scale = jnp.exp(jax.random.uniform(col_key, (1, D), jnp.float32, 0.0, jnp.log(10.0)))
    return values * row_scale * ramp[:, None] * col_scale / 10.0


def draw_activations(key, part):
    return scaled_draw(jax.random.fold_in(key, 11)).astype(jnp.bfloat16)


def draw_out_grads(key, part):
    return scaled_draw(jax.random.fold_in(key, 23)).astype(jnp.bfloat16)


def setup_inputs(seed: int = 0) -> dict:
    streams_of = jax.random.split(jax.random.key(seed), 3)
    activations = draw_activations(jax.random.fold_in(streams_of[2], 71), 0)
    out_grads = draw_out_grads(jax.random.fold_in(streams_of[2], 71), 0)
    return dict(activations=activations, out_grads=out_grads)


damping = 0.3
epsilon = 1e-06
divisor = 2.0

def factor_gram(data):
    shards = data.reshape(N_TOK, TOK_DEV, D)

    def add_shard(total, shard):
        partial_value = jnp.dot(shard.T, shard, preferred_element_type=jnp.float32)
        rounded = lax.optimization_barrier(partial_value.astype(jnp.bfloat16))
        return (total + rounded.astype(jnp.float32), None)
    total, unused = lax.scan(add_shard, jnp.zeros((D, D), jnp.float32), shards)
    return total

def factor_inverse(data):
    gram = factor_gram(data)
    values = data.astype(jnp.float32)
    sums = lax.optimization_barrier(jnp.sum(values * values, axis=0))
    inverse = lax.rsqrt(sums / TOKENS + epsilon)
    identity = jnp.eye(D, dtype=jnp.float32)
    damped = gram / TOKENS * inverse[:, None] * inverse[None, :] + damping * identity
    scaled = damped / divisor
    half = scaled.astype(jnp.bfloat16)
    square = jnp.dot(half, half, preferred_element_type=jnp.float32)
    cube = jnp.dot(half, square.astype(jnp.bfloat16), preferred_element_type=jnp.float32)
    return 4.0 * identity - 6.0 * scaled + 4.0 * square - cube

def reference(activations, out_grads):
    return (factor_inverse(activations), factor_inverse(out_grads))
```

```python
import jax
import jax.numpy as jnp
from jax import lax
from jax.sharding import Mesh, PartitionSpec as P

D = 4096
TOKENS = 8192
damping = 0.3
epsilon = 1e-06
divisor = 2.0

CENTER = 2.0 / 3.0
P0 = 4.0 - 6.0 * CENTER + 4.0 * CENTER**2 - CENTER**3
P1 = -6.0 + 8.0 * CENTER - 3.0 * CENTER**2
P2 = 4.0 - 3.0 * CENTER

NAMES = ("zlo", "y", "core", "x", "zhi")
TOK = ("zlo", "y", "core")
BLK = ("x", "zhi")
Z = ("zhi", "zlo")
f32 = jnp.float32
bf16 = jnp.bfloat16


def exchange(pieces, axes):
    return lax.all_to_all(pieces, axes, 0, 0, tiled=True)


def gathered(value, axes):
    count = lax.axis_size(axes)
    return exchange(jnp.broadcast_to(value[None], (count, *value.shape)), axes)


def summed(pieces):
    return jnp.sum(pieces.astype(f32), axis=0)


def other_core(value):
    return lax.ppermute(value, "core", [(0, 1), (1, 0)])


def role_swap():
    pairs = []
    for x in range(4):
        for y in range(4):
            for zhi in range(2):
                source = (y * 4 + x) * 2 + zhi
                to_y = (y // 2) * 2 + zhi
                to_x = (y % 2) * 2 + x // 2
                pairs.append((source, (to_y * 4 + to_x) * 2 + x % 2))
    return pairs


def body(activations, out_grads):
    zlo, y, core = (lax.axis_index(a) for a in TOK)
    x, zhi = (lax.axis_index(a) for a in BLK)
    block = zlo * 16 + (y // 2) * 8 + zhi * 4 + core * 2 + y % 2
    row_ids = block * 128 + jnp.arange(128, dtype=jnp.int32)
    col_ids = x * 1024 + jnp.arange(1024, dtype=jnp.int32)
    both = (activations, out_grads)

    squares = jnp.stack([jnp.sum(jnp.square(v.astype(f32)), axis=0) for v in both])
    sums = jnp.sum(gathered(squares, TOK), axis=0)
    inverse = gathered(lax.rsqrt(sums / TOKENS + epsilon), BLK)
    inverse = jnp.moveaxis(inverse, 0, 1).reshape(2, D)

    results = []
    for k, data in enumerate(both):
        cols = gathered(data, "zhi")
        rows = gathered(data, "x")
        product = lax.dot_general(
            rows, cols, (((1,), (1,)), ((), ())), preferred_element_type=f32
        )
        product = product.astype(bf16).reshape(4, 2, 256, 1024)
        kept = lax.dynamic_index_in_dim(product, core, 1, keepdims=False)
        sent = lax.dynamic_index_in_dim(product, 1 - core, 1, keepdims=False)
        pair = (kept.astype(f32) + other_core(sent).astype(f32)).astype(bf16)
        gram = summed(exchange(pair.reshape(8, 128, 1024), ("zlo", "y")))

        inverse_rows = lax.dynamic_slice_in_dim(inverse[k], block * 128, 128)
        inverse_cols = lax.dynamic_slice_in_dim(inverse[k], x * 1024, 1024)
        eye = (row_ids[:, None] == col_ids[None, :]).astype(f32)
        shifted = (
            gram * (inverse_rows / (TOKENS * divisor))[:, None] * inverse_cols[None, :]
            + (damping / divisor - CENTER) * eye
        )
        half = shifted.astype(bf16)

        left = gathered(half, "y").reshape(512, 1024)
        mine = gathered(half, Z).reshape(512, 1024)
        theirs = other_core(mine)
        right = jnp.concatenate([mine, theirs])
        square = lax.dot_general(
            left, right, (((1,), (1,)), ((), ())), preferred_element_type=f32
        ).astype(bf16)
        square = summed(exchange(square.reshape(4, 128, 1024), "x")).astype(bf16)
        square = gathered(square, "x").reshape(512, 1024)

        z_block = jnp.arange(4, dtype=jnp.int32)
        of_z = (z_block % 2) * 16 + (z_block // 2) * 4 + (y // 2) * 8 + y % 2
        of_core = jnp.stack([core, 1 - core]) * 2
        blocks = (of_core[:, None] + of_z[None, :]).reshape(8)
        right_ids = (blocks[:, None] * 128 + jnp.arange(128, dtype=jnp.int32)).reshape(1024)
        right_eye = (right_ids[:, None] == col_ids[None, :]).astype(f32)
        factor = (P2 * right_eye - right.astype(f32)).astype(bf16)
        tail = jnp.dot(square, factor, preferred_element_type=f32).astype(bf16)
        tail = summed(exchange(tail.reshape(4, 128, 1024), "y"))

        result = (P1 * shifted + tail).astype(bf16).reshape(4, 32, 1024)
        result = exchange(result, "x")
        result = lax.ppermute(result, ("y", "x", "zhi"), role_swap())
        out = jnp.moveaxis(result, 0, 1).reshape(32, D).astype(f32)
        out_ids = (((zlo * 4 + y) * 2 + core) * 8 + x * 2 + zhi) * 32 + jnp.arange(
            32, dtype=jnp.int32
        )
        out_eye = out_ids[:, None] == jnp.arange(D, dtype=jnp.int32)[None, :]
        results.append(out + P0 * out_eye.astype(f32))
    return tuple(results)


def solution(mesh):
    split = Mesh(mesh.devices.reshape(2, 4, 2, 4, 2), NAMES)
    placed = P(TOK, BLK)
    return jax.shard_map(
        body,
        mesh=split,
        in_specs=(placed, placed),
        out_specs=(P(NAMES, None), P(NAMES, None)),
        check_vma=False,
    )
```

```python
import jax
import jax.numpy as jnp
from jax import lax
from jax.experimental import pallas as pl
from jax.experimental.pallas import tpu as pltpu
from jax.sharding import Mesh, PartitionSpec as P

D = 4096
TOKENS = 8192
damping = 0.3
epsilon = 1e-06
divisor = 2.0

CENTER = 2.0 / 3.0
P0 = 4.0 - 6.0 * CENTER + 4.0 * CENTER**2 - CENTER**3
P1 = -6.0 + 8.0 * CENTER - 3.0 * CENTER**2
P2 = 4.0 - 3.0 * CENTER

NAMES = ("zlo", "y", "core", "x", "zhi")
TOK = ("zlo", "y", "core")
BLK = ("x", "zhi")
Z = ("zlo", "zhi")
STEPS = (1, -1, 2)
f32 = jnp.float32
bf16 = jnp.bfloat16
WHOLE = pl.BlockSpec(memory_space=pltpu.VMEM)
SCALARS = pl.BlockSpec(memory_space=pltpu.SMEM)
ANYWHERE = pl.BlockSpec(memory_space=pl.ANY)


def exchange(pieces, axes):
    return lax.all_to_all(pieces, axes, 0, 0, tiled=True)


def gathered(value, axes):
    count = lax.axis_size(axes)
    return exchange(jnp.broadcast_to(value[None], (count, *value.shape)), axes)


def shifted_by(value, axis, step):
    place = (lambda z: (z % 2) * 2 + z // 2) if axis == Z else (lambda i: i)
    return lax.ppermute(value, axis, [(place(i), place((i + step) % 4)) for i in range(4)])


def from_ring(value, axis):
    return [value] + [shifted_by(value, axis, step) for step in STEPS]


def ring_sum(pieces, axis):
    got = [pieces[0]] + [shifted_by(pieces[k], axis, k) for k in range(1, 4)]
    return sum(piece.astype(f32) for piece in got)


def other_core(value):
    return lax.ppermute(value, "core", [(0, 1), (1, 0)])


def other_zhi(value):
    return lax.ppermute(value, "zhi", [(0, 1), (1, 0)])


def call(kernel, outs, operands, specs, scratch=(), flops=0, moved=0, name=None):
    return pl.pallas_call(
        kernel,
        out_shape=outs,
        in_specs=specs,
        out_specs=jax.tree.map(lambda _: WHOLE, outs),
        scratch_shapes=list(scratch),
        compiler_params=pltpu.CompilerParams(vmem_limit_bytes=40 * 1024 * 1024),
        cost_estimate=pl.CostEstimate(flops=flops, bytes_accessed=moved, transcendentals=0),
        name=name,
    )(*operands)


def gram_kernel(ids, b0, b1, b2, b3, own, other, kept, sent):
    x, core, zhi = ids[0], ids[2], ids[4]
    first = zhi == 0
    a = jnp.concatenate(
        [
            jnp.where(first, own[...], other[...]),
            jnp.where(first, other[...], own[...]),
        ],
        axis=1,
    )
    for ref, step in zip((b0, b1, b2, b3), (0, *STEPS)):
        source = lax.rem(x - step + 4, 4)
        for out, which in ((sent, 1 - core), (kept, core)):
            rows = ref[pl.ds(pl.multiple_of(which * 256, 256), 256), :]
            out[source] = jnp.dot(rows, a, preferred_element_type=f32).astype(bf16)


def gram_product(ids, shards, own, other):
    out = jax.ShapeDtypeStruct((4, 256, 1024), bf16)
    return call(
        gram_kernel,
        (out, out),
        (ids, *shards, own, other),
        [SCALARS] + [WHOLE] * 6,
        flops=2 * 512 * 1024 * 2048,
        moved=7 << 20,
        name="gram",
    )


def square_kernel(ids, *refs):
    lefts, rights, outs = refs[:4], refs[4:12], refs[12:16]
    left, right, sems = refs[16:]
    x, y, z = ids[0], ids[1], ids[4] * 2 + ids[3]
    copies = []
    for k, (ref, step) in enumerate(zip(lefts, (0, *STEPS))):
        slot = lax.rem(y - step - x + 8, 4)
        copies.append(
            pltpu.make_async_copy(
                ref, left.at[pl.ds(pl.multiple_of(slot * 128, 128), 128)], sems.at[k]
            )
        )
    for k, ref in enumerate(rights):
        slot = (k // 4) * 4 + lax.rem(z - (0, *STEPS)[k % 4] + 4, 4)
        copies.append(
            pltpu.make_async_copy(
                ref, right.at[pl.ds(pl.multiple_of(slot * 128, 128), 128)], sems.at[4 + k]
            )
        )
    for copy in copies:
        copy.start()
    for copy in copies:
        copy.wait()
    product = lax.dot_general(
        left[...], right[...], (((1,), (1,)), ((), ())), preferred_element_type=f32
    ).astype(bf16)
    for k, out in enumerate(outs):
        out[...] = product[k * 128 : (k + 1) * 128]


def square_pieces(ids, lefts, rights):
    out = jax.ShapeDtypeStruct((128, 1024), bf16)
    return call(
        square_kernel,
        (out,) * 4,
        (ids, *lefts, *rights),
        [SCALARS] + [ANYWHERE] * 12,
        scratch=[
            pltpu.VMEM((512, 1024), bf16),
            pltpu.VMEM((1024, 1024), bf16),
            pltpu.SemaphoreType.DMA((12,)),
        ],
        flops=2 * 512 * 1024 * 1024,
        moved=4 << 20,
        name="square",
    )


def cube_kernel(ids, squares, half_own, half_other, *refs):
    rights, outs = refs[:8], refs[8:12]
    factor, total = refs[12:]
    x, y, core, zlo, zhi = (ids[k] for k in range(5))
    row = lax.broadcasted_iota(jnp.int32, (128, 1024), 0)
    col = lax.broadcasted_iota(jnp.int32, (128, 1024), 1)
    z = zhi * 2 + zlo
    for k, ref in enumerate(rights):
        of_core = core if k < 4 else 1 - core
        of_z = lax.rem(z - (0, *STEPS)[k % 4] + 4, 4)
        of_zlo, of_zhi = lax.rem(of_z, 2), lax.div(of_z, 2)
        block = of_zlo * 16 + lax.div(y, 2) * 8 + of_zhi * 4 + of_core * 2 + lax.rem(y, 2)
        diagonal = row + (block * 128 - x * 1024) == col
        slot = (k // 4) * 4 + of_z
        factor[pl.ds(pl.multiple_of(slot * 128, 128), 128)] = (
            jnp.where(diagonal, P2, 0.0) - ref[...].astype(f32)
        ).astype(bf16)
    total[...] = jnp.dot(squares[...], factor[...], preferred_element_type=f32)
    for other in range(2):
        half = (half_own, half_other)[other]
        f9 = zhi if other == 0 else 1 - zhi
        place = pl.ds(pl.multiple_of((y * 2 + f9) * 64, 64), 64)
        total[place] += P1 * half[...].astype(f32)
    for k, out in enumerate(outs):
        to_y = lax.rem(y + k, 4)
        for f7 in range(2):
            at = ((lax.div(to_y, 2) * 2 + f7) * 2 + lax.rem(to_y, 2)) * 64
            out[f7 * 64 : (f7 + 1) * 64] = total[pl.ds(pl.multiple_of(at, 64), 64)].astype(bf16)


def cube_pieces(ids, squares, half_own, half_other, rights):
    out = jax.ShapeDtypeStruct((128, 1024), bf16)
    return call(
        cube_kernel,
        (out,) * 4,
        (ids, squares, half_own, half_other, *rights),
        [SCALARS] + [WHOLE] * 11,
        scratch=[pltpu.VMEM((1024, 1024), bf16), pltpu.VMEM((512, 1024), f32)],
        flops=2 * 512 * 1024 * 1024,
        moved=4 << 20,
        name="cube",
    )


def out_kernel(ids, *refs):
    pieces, out = refs[:4], refs[4]
    x, y, core, zlo, zhi = (ids[k] for k in range(5))
    first = (((zlo * 4 + y) * 2 + core) * 8 + x * 2 + zhi) * 32
    row = lax.broadcasted_iota(jnp.int32, (32, 1024), 0)
    col = lax.broadcasted_iota(jnp.int32, (32, 1024), 1)
    for k, ref in enumerate(pieces):
        source = lax.rem(x - k + 4, 4)
        diagonal = row + (first - source * 1024) == col
        out[:, pl.ds(pl.multiple_of(source * 1024, 1024), 1024)] = ref[...].astype(
            f32
        ) + jnp.where(diagonal, P0, 0.0)


def assembled(ids, pieces):
    return call(
        out_kernel,
        jax.ShapeDtypeStruct((32, D), f32),
        (ids, *pieces),
        [SCALARS] + [WHOLE] * 4,
        flops=2 * 32 * D,
        moved=1 << 20,
        name="assemble",
    )


def body(activations, out_grads):
    zlo, y, core = (lax.axis_index(a) for a in TOK)
    x, zhi = (lax.axis_index(a) for a in BLK)
    ids = jnp.stack([x, y, core, zlo, zhi]).astype(jnp.int32)
    block = zlo * 16 + (y // 2) * 8 + zhi * 4 + core * 2 + y % 2
    row_ids = block * 128 + jnp.arange(128, dtype=jnp.int32)
    col_ids = x * 1024 + jnp.arange(1024, dtype=jnp.int32)
    eye = (row_ids[:, None] == col_ids[None, :]).astype(f32)
    both = (activations, out_grads)

    squares = jnp.stack([jnp.sum(jnp.square(v.astype(f32)), axis=0) for v in both])
    sums = jnp.sum(gathered(squares, TOK), axis=0)
    inverse = gathered(lax.rsqrt(sums / TOKENS + epsilon), BLK)
    inverse = jnp.moveaxis(inverse, 0, 1).reshape(2, D)

    results = []
    for n, data in enumerate(both):
        shards = from_ring(data.T, "x")
        kept, sent = gram_product(ids, shards, data, other_zhi(data))
        pair = (kept.astype(f32) + other_core(sent).astype(f32)).astype(bf16)
        pieces = exchange(pair.reshape(8, 128, 1024), ("zlo", "y"))
        gram = jnp.sum(pieces.astype(f32), axis=0)

        inverse_rows = lax.dynamic_slice_in_dim(inverse[n], block * 128, 128)
        inverse_cols = lax.dynamic_slice_in_dim(inverse[n], x * 1024, 1024)
        half = (
            gram * (inverse_rows / (TOKENS * divisor))[:, None] * inverse_cols[None, :]
            + (damping / divisor - CENTER) * eye
        ).astype(bf16)
        by_f5 = half.reshape(2, 2, 32, 1024)
        half_own = lax.dynamic_index_in_dim(by_f5, zhi, 1, keepdims=False).reshape(64, 1024)
        half_away = lax.dynamic_index_in_dim(by_f5, 1 - zhi, 1, keepdims=False)
        half_other = other_zhi(half_away.reshape(64, 1024))

        lefts = from_ring(half, "y")
        mine = from_ring(half, Z)
        rights = mine + [other_core(piece) for piece in mine]
        square = ring_sum(square_pieces(ids, lefts, rights), "x").astype(bf16)
        square = jnp.moveaxis(square.reshape(2, 2, 32, 1024), 1, 0).reshape(1, 2, 64, 1024)
        square = jnp.broadcast_to(square, (4, 2, 64, 1024)).reshape(8, 64, 1024)
        square = exchange(square, BLK).reshape(512, 1024)
        tail = ring_sum(cube_pieces(ids, square, half_own, half_other, rights), "y")
        tail = tail.astype(bf16).reshape(4, 32, 1024)

        outs = [
            lax.dynamic_index_in_dim(tail, (x + k) % 4, 0, keepdims=False) for k in range(4)
        ]
        outs = [outs[0]] + [shifted_by(outs[k], "x", k) for k in range(1, 4)]
        results.append(assembled(ids, outs))
    return tuple(results)


def solution(mesh):
    split = Mesh(mesh.devices.reshape(2, 4, 2, 4, 2), NAMES)
    placed = P(TOK, BLK)
    return jax.shard_map(
        body,
        mesh=split,
        in_specs=(placed, placed),
        out_specs=(P(NAMES, None), P(NAMES, None)),
        check_vma=False,
    )
```

```python
import functools

import jax
import jax.numpy as jnp
from jax import lax
from jax.experimental import pallas as pl
from jax.experimental.pallas import tpu as pltpu
from jax.sharding import Mesh, PartitionSpec as P


D = 4096
TOKENS = 8192
damping = 0.3
epsilon = 1e-06
divisor = 2.0

CENTER = 2.0 / 3.0
P0 = 4.0 - 6.0 * CENTER + 4.0 * CENTER**2 - CENTER**3
P1 = -6.0 + 8.0 * CENTER - 3.0 * CENTER**2
P2 = 4.0 - 3.0 * CENTER

NAMES = ("zlo", "y", "core", "x", "zhi")
TOK = ("zlo", "y", "core")
BLK = ("x", "zhi")
Z = ("zlo", "zhi")
STEPS = (1, -1, 2)
f32 = jnp.float32
bf16 = jnp.bfloat16
WHOLE = pl.BlockSpec(memory_space=pltpu.VMEM)
SCALARS = pl.BlockSpec(memory_space=pltpu.SMEM)
ANYWHERE = pl.BlockSpec(memory_space=pl.ANY)


def exchange(pieces, axes):
    return lax.all_to_all(pieces, axes, 0, 0, tiled=True)


def gathered(value, axes):
    count = lax.axis_size(axes)
    return exchange(jnp.broadcast_to(value[None], (count, *value.shape)), axes)


def shifted_by(value, axis, step):
    place = (lambda z: (z % 2) * 2 + z // 2) if axis == Z else (lambda i: i)
    return lax.ppermute(value, axis, [(place(i), place((i + step) % 4)) for i in range(4)])


def from_ring(value, axis):
    return [value] + [shifted_by(value, axis, step) for step in STEPS]


def ring_sum(pieces, axis):
    got = [pieces[0]] + [shifted_by(pieces[k], axis, k) for k in range(1, 4)]
    return sum(piece.astype(f32) for piece in got)


def other_core(value):
    return lax.ppermute(value, "core", [(0, 1), (1, 0)])


def other_zhi(value):
    return lax.ppermute(value, "zhi", [(0, 1), (1, 0)])


def call(kernel, outs, operands, specs, scratch=(), flops=0, moved=0):
    return pl.pallas_call(
        kernel,
        out_shape=outs,
        in_specs=specs,
        out_specs=jax.tree.map(lambda _: WHOLE, outs),
        scratch_shapes=list(scratch),
        compiler_params=pltpu.CompilerParams(vmem_limit_bytes=40 * 1024 * 1024),
        cost_estimate=pl.CostEstimate(flops=flops, bytes_accessed=moved, transcendentals=0),
    )(*operands)


def gram_kernel(keep, ids, *refs):
    shards, own, other = refs[:4], refs[4], refs[5]
    received = refs[6] if keep else None
    out, b, a, added, sems = refs[-5:]
    x, core, zhi = ids[0], ids[2], ids[4]
    which = core if keep else 1 - core
    rows = pl.ds(pl.multiple_of(which * 256, 256), 256)
    copies = [
        pltpu.make_async_copy(own, a.at[zhi], sems.at[4]),
        pltpu.make_async_copy(other, a.at[1 - zhi], sems.at[5]),
    ]
    for k, ref in enumerate(shards):
        copies.append(pltpu.make_async_copy(ref.at[rows], b.at[k], sems.at[k]))
    if keep:
        copies.append(pltpu.make_async_copy(received, added, sems.at[6]))
    for copy in copies:
        copy.start()
    for copy in copies:
        copy.wait()
    for k, step in enumerate((0, *STEPS)):
        source = lax.rem(x - step + 4, 4)
        for half in range(2):
            cols = slice(half * 512, (half + 1) * 512)
            piece = jnp.dot(b[k], a[half], preferred_element_type=f32).astype(bf16)
            if keep:
                piece = (piece.astype(f32) + added[source, :, cols].astype(f32)).astype(bf16)
            out[source, :, cols] = piece


def gram_half(keep, ids, shards, own, other, received=()):
    return call(
        functools.partial(gram_kernel, keep),
        jax.ShapeDtypeStruct((4, 256, 1024), bf16),
        (ids, *shards, own, other, *received),
        [SCALARS] + [ANYWHERE] * (6 + keep),
        scratch=[
            pltpu.VMEM((4, 256, 512), bf16),
            pltpu.VMEM((2, 512, 512), bf16),
            pltpu.VMEM((4, 256, 1024) if keep else (8, 128), bf16),
            pltpu.SemaphoreType.DMA((7,)),
        ],
        flops=512 * 1024 * 2048,
        moved=7 << 20,
    )


def half_kernel(ids, pieces, by_row, by_col, half, own, away):
    x, y, core, zlo, zhi = (ids[k] for k in range(5))
    block = zlo * 16 + lax.div(y, 2) * 8 + zhi * 4 + core * 2 + lax.rem(y, 2)
    for part in range(4):
        f5 = part % 2
        rows = slice(part * 32, part * 32 + 32)
        row = lax.broadcasted_iota(jnp.int32, (32, 1024), 0) + part * 32
        col = lax.broadcasted_iota(jnp.int32, (32, 1024), 1)
        diagonal = row + (block * 128 - x * 1024) == col
        gram = pieces[0, rows].astype(f32)
        for k in range(1, 8):
            gram += pieces[k, rows].astype(f32)
        value = gram * by_row[rows, :1] * by_col[...]
        value += jnp.where(diagonal, damping / divisor - CENTER, 0.0)
        value = value.astype(bf16)
        half[rows] = value
        place = slice(part // 2 * 32, part // 2 * 32 + 32)

        @pl.when(zhi == f5)
        def _():
            own[place] = value

        @pl.when(zhi != f5)
        def _():
            away[place] = value


def halves(ids, pieces, by_row, by_col):
    small = jax.ShapeDtypeStruct((64, 1024), bf16)
    return call(
        half_kernel,
        (jax.ShapeDtypeStruct((128, 1024), bf16), small, small),
        (ids, pieces, by_row, by_col),
        [SCALARS] + [WHOLE] * 3,
        flops=20 * 128 * 1024,
        moved=3 << 20,
    )


def square_kernel(ids, *refs):
    lefts, rights, outs = refs[:4], refs[4:12], refs[12:16]
    left, right, sems = refs[16:]
    x, y, z = ids[0], ids[1], ids[4] * 2 + ids[3]
    copies = []
    for k, (ref, step) in enumerate(zip(lefts, (0, *STEPS))):
        slot = lax.rem(y - step - x + 8, 4)
        copies.append(
            pltpu.make_async_copy(
                ref, left.at[pl.ds(pl.multiple_of(slot * 128, 128), 128)], sems.at[k]
            )
        )
    for k, ref in enumerate(rights):
        slot = (k // 4) * 4 + lax.rem(z - (0, *STEPS)[k % 4] + 4, 4)
        copies.append(
            pltpu.make_async_copy(
                ref, right.at[pl.ds(pl.multiple_of(slot * 128, 128), 128)], sems.at[4 + k]
            )
        )
    for copy in copies:
        copy.start()
    for copy in copies:
        copy.wait()
    product = lax.dot_general(
        left[...], right[...], (((1,), (1,)), ((), ())), preferred_element_type=f32
    ).astype(bf16)
    for k, out in enumerate(outs):
        out[...] = product[k * 128 : (k + 1) * 128]


def square_pieces(ids, lefts, rights):
    out = jax.ShapeDtypeStruct((128, 1024), bf16)
    return call(
        square_kernel,
        (out,) * 4,
        (ids, *lefts, *rights),
        [SCALARS] + [ANYWHERE] * 12,
        scratch=[
            pltpu.VMEM((512, 1024), bf16),
            pltpu.VMEM((1024, 1024), bf16),
            pltpu.SemaphoreType.DMA((12,)),
        ],
        flops=2 * 512 * 1024 * 1024,
        moved=4 << 20,
    )


def factor_kernel(ids, *refs):
    rights, out, right, sems = refs[:8], refs[8], refs[9], refs[10]
    x, y, core, zlo, zhi = (ids[k] for k in range(5))
    copies = [pltpu.make_async_copy(ref, right.at[k], sems.at[k]) for k, ref in enumerate(rights)]
    for copy in copies:
        copy.start()
    for copy in copies:
        copy.wait()
    row = lax.broadcasted_iota(jnp.int32, (128, 1024), 0)
    col = lax.broadcasted_iota(jnp.int32, (128, 1024), 1)
    z = zhi * 2 + zlo
    for k in range(8):
        of_core = core if k < 4 else 1 - core
        of_z = lax.rem(z - (0, *STEPS)[k % 4] + 4, 4)
        of_zlo, of_zhi = lax.rem(of_z, 2), lax.div(of_z, 2)
        block = of_zlo * 16 + lax.div(y, 2) * 8 + of_zhi * 4 + of_core * 2 + lax.rem(y, 2)
        diagonal = row + (block * 128 - x * 1024) == col
        slot = (k // 4) * 4 + of_z
        out[pl.ds(pl.multiple_of(slot * 128, 128), 128)] = (
            jnp.where(diagonal, P2, 0.0) - right[k].astype(f32)
        ).astype(bf16)


def factor_of(ids, rights):
    return call(
        factor_kernel,
        jax.ShapeDtypeStruct((1024, 1024), bf16),
        (ids, *rights),
        [SCALARS] + [ANYWHERE] * 8,
        scratch=[pltpu.VMEM((8, 128, 1024), bf16), pltpu.SemaphoreType.DMA((8,))],
        flops=4 * 1024 * 1024,
        moved=4 << 20,
    )


def cube_kernel(ids, squares_in, half_own, half_other, factor_in, *refs):
    outs = refs[:4]
    factor, total, squares, halves, sems = refs[4:]
    y, zhi = ids[1], ids[4]
    copies = [
        pltpu.make_async_copy(half_own, halves.at[0], sems.at[0]),
        pltpu.make_async_copy(half_other, halves.at[1], sems.at[1]),
        pltpu.make_async_copy(squares_in, squares, sems.at[2]),
        pltpu.make_async_copy(factor_in, factor, sems.at[3]),
    ]
    for copy in copies:
        copy.start()
    for copy in copies:
        copy.wait()
    total[...] = jnp.dot(squares[...], factor[...], preferred_element_type=f32)
    for other in range(2):
        f9 = zhi if other == 0 else 1 - zhi
        place = pl.ds(pl.multiple_of((y * 2 + f9) * 64, 64), 64)
        total[place] += P1 * halves[other].astype(f32)
    for k, out in enumerate(outs):
        to_y = lax.rem(y + k, 4)
        for f7 in range(2):
            at = ((lax.div(to_y, 2) * 2 + f7) * 2 + lax.rem(to_y, 2)) * 64
            out[f7 * 64 : (f7 + 1) * 64] = total[pl.ds(pl.multiple_of(at, 64), 64)].astype(bf16)


def cube_pieces(ids, squares, half_own, half_other, factor):
    out = jax.ShapeDtypeStruct((128, 1024), bf16)
    return call(
        cube_kernel,
        (out,) * 4,
        (ids, squares, half_own, half_other, factor),
        [SCALARS] + [ANYWHERE] * 4,
        scratch=[
            pltpu.VMEM((1024, 1024), bf16),
            pltpu.VMEM((512, 1024), f32),
            pltpu.VMEM((512, 1024), bf16),
            pltpu.VMEM((2, 64, 1024), bf16),
            pltpu.SemaphoreType.DMA((4,)),
        ],
        flops=2 * 512 * 1024 * 1024,
        moved=4 << 20,
    )


def out_kernel(ids, *refs):
    pieces, out = refs[:4], refs[4]
    x, y, core, zlo, zhi = (ids[k] for k in range(5))
    first = (((zlo * 4 + y) * 2 + core) * 8 + x * 2 + zhi) * 32
    row = lax.broadcasted_iota(jnp.int32, (32, 1024), 0)
    col = lax.broadcasted_iota(jnp.int32, (32, 1024), 1)
    for k, ref in enumerate(pieces):
        source = lax.rem(x - k + 4, 4)
        diagonal = row + (first - source * 1024) == col
        out[:, pl.ds(pl.multiple_of(source * 1024, 1024), 1024)] = ref[...].astype(
            f32
        ) + jnp.where(diagonal, P0, 0.0)


def assembled(ids, pieces):
    return call(
        out_kernel,
        jax.ShapeDtypeStruct((32, D), f32),
        (ids, *pieces),
        [SCALARS] + [WHOLE] * 4,
        flops=2 * 32 * D,
        moved=1 << 20,
    )


def body(activations, out_grads):
    zlo, y, core = (lax.axis_index(a) for a in TOK)
    x, zhi = (lax.axis_index(a) for a in BLK)
    ids = jnp.stack([x, y, core, zlo, zhi]).astype(jnp.int32)
    block = zlo * 16 + (y // 2) * 8 + zhi * 4 + core * 2 + y % 2
    both = (activations, out_grads)

    def inverses():
        squares = jnp.stack([jnp.sum(jnp.square(v.astype(f32)), axis=0) for v in both])
        sums = jnp.sum(gathered(squares, TOK), axis=0)
        inverse = gathered(lax.rsqrt(sums / TOKENS + epsilon), BLK)
        return jnp.moveaxis(inverse, 0, 1).reshape(2, D)

    inverse = inverses()
    by_row = lax.dynamic_slice_in_dim(inverse, block * 128, 128, axis=1)
    by_row = jnp.broadcast_to(by_row[:, :, None] / (TOKENS * divisor), (2, 128, 128))
    by_col = lax.dynamic_slice_in_dim(inverse, x * 1024, 1024, axis=1)[:, None]
    results = []
    for n, data in enumerate(both):
        shards = from_ring(data.T, "x")
        away = other_zhi(data)
        sent = gram_half(False, ids, shards, data, away)
        received = other_core(sent)
        pair = gram_half(True, ids, shards, data, away, (received,))
        pieces = exchange(pair.reshape(8, 128, 1024), ("zlo", "y"))
        half, half_own, half_away = halves(ids, pieces, by_row[n], by_col[n])
        mine = from_ring(half, Z)
        lefts = from_ring(half, "y")
        half_other = other_zhi(half_away)
        rights = mine + [other_core(piece) for piece in mine]
        parts = square_pieces(ids, lefts, rights)
        factor = factor_of(ids, rights)
        square = ring_sum(parts, "x").astype(bf16)
        square = jnp.moveaxis(square.reshape(2, 2, 32, 1024), 1, 0).reshape(1, 2, 64, 1024)
        square = jnp.broadcast_to(square, (4, 2, 64, 1024)).reshape(8, 64, 1024)
        square = exchange(square, BLK).reshape(512, 1024)
        parts = cube_pieces(ids, square, half_own, half_other, factor)
        tail = ring_sum(parts, "y")
        tail = tail.astype(bf16).reshape(4, 32, 1024)
        outs = [
            lax.dynamic_index_in_dim(tail, (x + k) % 4, 0, keepdims=False) for k in range(4)
        ]
        outs = [outs[0]] + [shifted_by(outs[k], "x", k) for k in range(1, 4)]
        results.append(assembled(ids, outs))
    return tuple(results)


def solution(mesh):
    split = Mesh(mesh.devices.reshape(2, 4, 2, 4, 2), NAMES)
    placed = P(TOK, BLK)
    return jax.shard_map(
        body,
        mesh=split,
        in_specs=(placed, placed),
        out_specs=(P(NAMES, None), P(NAMES, None)),
        check_vma=False,
    )
```

```python
import functools

import jax
import jax.numpy as jnp
from jax import lax
from jax.experimental import pallas as pl
from jax.experimental.pallas import tpu as pltpu
from jax.sharding import Mesh, PartitionSpec as P


D = 4096
TOKENS = 8192
damping = 0.3
epsilon = 1e-06
divisor = 2.0

CENTER = 2.0 / 3.0
P0 = 4.0 - 6.0 * CENTER + 4.0 * CENTER**2 - CENTER**3

NAMES = ("zlo", "y", "core", "x", "zhi")
TOK = ("zlo", "y", "core")
BLK = ("x", "zhi")
Z = ("zlo", "zhi")
STEPS = (1, -1, 2)
f32 = jnp.float32
bf16 = jnp.bfloat16
WHOLE = pl.BlockSpec(memory_space=pltpu.VMEM)
ANYWHERE = pl.BlockSpec(memory_space=pl.ANY)


def exchange(pieces, axes):
    return lax.all_to_all(pieces, axes, 0, 0, tiled=True)


def shifted_by(value, axis, step):
    place = (lambda z: (z % 2) * 2 + z // 2) if axis == Z else (lambda i: i)
    return lax.ppermute(value, axis, [(place(i), place((i + step) % 4)) for i in range(4)])


def to_y_and_zlo(value, step, flip):
    pairs = [
        (zlo * 4 + y, (zlo ^ flip) * 4 + (y + step) % 4) for zlo in range(2) for y in range(4)
    ]
    return lax.ppermute(value, ("zlo", "y"), pairs)


def from_ring(value, axis):
    return [value] + [shifted_by(value, axis, step) for step in STEPS]


def along_ring(pieces, axis):
    return [pieces[0]] + [shifted_by(pieces[k], axis, k) for k in range(1, 4)]


def other_core(value):
    return lax.ppermute(value, "core", [(0, 1), (1, 0)])


def other_zhi(value):
    return lax.ppermute(value, "zhi", [(0, 1), (1, 0)])


def position():
    return [lax.axis_index(a) for a in ("x", "y", "core", "zlo", "zhi")]


def call(kernel, outs, operands, specs, scratch=(), flops=0, moved=0, to=WHOLE):
    return pl.pallas_call(
        kernel,
        out_shape=outs,
        in_specs=specs,
        out_specs=jax.tree.map(lambda _: to, outs),
        scratch_shapes=list(scratch),
        compiler_params=pltpu.CompilerParams(vmem_limit_bytes=12 * 1024 * 1024),
        cost_estimate=pl.CostEstimate(flops=flops, bytes_accessed=moved, transcendentals=0),
    )(*operands)


def three_parts(value):
    high = value.astype(bf16).astype(f32)
    rest = value - high
    middle = rest.astype(bf16).astype(f32)
    return high, middle, rest - middle


def sum_rows(of_cols, of_rows):
    row = lax.broadcasted_iota(jnp.int32, (8, 1024), 0)
    of_rows = jnp.concatenate([of_rows, jnp.zeros((1, 896), f32)], axis=1)
    packed = jnp.zeros((8, 1024), f32)
    for k, part in enumerate((*three_parts(of_cols), *three_parts(of_rows))):
        packed = jnp.where(row == k, part, packed)
    return packed.astype(bf16)


def gram_kernel(keep, apart, *refs):
    shards, own, other = refs[:4], refs[4], refs[5]
    received = refs[6] if keep else None
    outs = refs[6 + keep : -5]
    b, a, added, staged, sems = refs[-5:]
    x, y, core, zlo, zhi = position()
    which = core if keep else 1 - core
    rows = pl.ds(pl.multiple_of(which * 256, 256), 256)
    copies = [
        pltpu.make_async_copy(own, a.at[zhi], sems.at[4]),
        pltpu.make_async_copy(other, a.at[1 - zhi], sems.at[5]),
    ]
    arrivals, stores = [], []
    for k, (ref, step) in enumerate(zip(shards, (0, *STEPS))):
        source = lax.rem(x - step + 4, 4)
        needed = [pltpu.make_async_copy(ref.at[rows], b.at[k], sems.at[k])]
        if keep:
            needed.append(pltpu.make_async_copy(received.at[source], added.at[k], sems.at[10 + k]))
        arrivals.append(needed)
    for copy in copies + [copy for needed in arrivals for copy in needed]:
        copy.start()
    for copy in copies:
        copy.wait()
    of_cols = jnp.concatenate(
        [jnp.sum(jnp.square(a[h].astype(f32)), axis=0, keepdims=True) for h in range(2)], axis=1
    )

    def one_shard(k, carry):
        source = lax.rem(x - jnp.where(k == 2, 3, jnp.where(k == 3, 2, k)) + 4, 4)
        pltpu.make_async_copy(shards[0].at[rows], b.at[k], sems.at[k]).wait()
        if keep:
            pltpu.make_async_copy(received.at[source], added.at[k], sems.at[10 + k]).wait()
        for half in range(2):
            cols = slice(half * 512, (half + 1) * 512)
            piece = jnp.dot(b[k], a[half], preferred_element_type=f32).astype(bf16)
            for part in range(2):
                value = piece[part * 128 : (part + 1) * 128]
                if keep:
                    value = value.astype(f32) + added[k, part, :128, cols].astype(f32)
                staged[source, part, :128, cols] = value.astype(bf16)
        squares = jnp.square(b[k].astype(f32))
        squares = sum(squares[:, q * 128 : (q + 1) * 128] for q in range(4))
        for part in range(2):
            of_rows = jnp.sum(squares[part * 128 : (part + 1) * 128].T, axis=0, keepdims=True)
            cols = of_cols
            if keep:
                more = added[k, part, 128:136].astype(f32)
                cols = cols + more[0:1] + more[1:2] + more[2:3]
                of_rows = of_rows + (more[3:4] + more[4:5] + more[5:6])[:, :128]
            staged[source, part, 128:136] = sum_rows(cols, of_rows)
        if not apart:
            pltpu.make_async_copy(staged.at[source], outs[0].at[source], sems.at[6 + k]).start()
        return carry

    lax.fori_loop(0, 4, one_shard, 0)
    if not apart:
        for k in range(4):
            stores.append(pltpu.make_async_copy(staged.at[k], outs[0].at[k], sems.at[6 + k]))
    if apart:
        for k, out in enumerate(outs):
            to_y = lax.rem(y + k % 4, 4)
            to_zlo = zlo if k < 4 else 1 - zlo
            piece = staged.at[to_zlo * 2 + lax.div(to_y, 2), lax.rem(to_y, 2)]
            stores.append(pltpu.make_async_copy(piece, out, sems.at[14 + k]))
            stores[-1].start()
    for copy in stores:
        copy.wait()


def gram_half(keep, apart, shards, own, other, received=()):
    shape = (4, 2, 136, 1024)
    if apart:
        out = (jax.ShapeDtypeStruct((136, 1024), bf16),) * 8
    else:
        out = pltpu.HBM(shape, bf16) if keep else jax.ShapeDtypeStruct(shape, bf16)
    return call(
        functools.partial(gram_kernel, keep, apart),
        out,
        (*shards, own, other, *received),
        [ANYWHERE] * (6 + keep),
        scratch=[
            pltpu.VMEM((4, 256, 512), bf16),
            pltpu.VMEM((2, 512, 512), bf16),
            pltpu.VMEM(shape if keep else (8, 128), bf16),
            pltpu.VMEM(shape, bf16),
            pltpu.SemaphoreType.DMA((22,)),
        ],
        to=ANYWHERE if apart else pl.BlockSpec(memory_space=pltpu.HBM),
        flops=512 * 1024 * 2048,
        moved=7 << 20,
    )


def half_kernel(*refs):
    half = refs[-1]
    pieces = refs[:-1] if len(refs) > 2 else [refs[0].at[k] for k in range(8)]
    x, y, core, zlo, zhi = position()
    block = zlo * 16 + lax.div(y, 2) * 8 + zhi * 4 + core * 2 + lax.rem(y, 2)
    sums = pieces[0][128:136].astype(f32)
    for k in range(1, 8):
        sums += pieces[k][128:136].astype(f32)
    by_col = lax.rsqrt((sums[0:1] + sums[1:2] + sums[2:3]) / TOKENS + epsilon)
    by_row = lax.rsqrt((sums[3:4] + sums[4:5] + sums[5:6])[:, :128] / TOKENS + epsilon)
    by_row = (jnp.broadcast_to(by_row, (128, 128)) / (TOKENS * divisor)).T[:, :1]
    for part in range(4):
        rows = slice(part * 32, part * 32 + 32)
        row = lax.broadcasted_iota(jnp.int32, (32, 1024), 0) + part * 32
        col = lax.broadcasted_iota(jnp.int32, (32, 1024), 1)
        diagonal = row + (block * 128 - x * 1024) == col
        gram = pieces[0][rows].astype(f32)
        for k in range(1, 8):
            gram += pieces[k][rows].astype(f32)
        value = gram * by_row[rows] * by_col
        value += jnp.where(diagonal, damping / divisor - CENTER, 0.0)
        value = value.astype(bf16)
        half[rows] = value


def halves(pieces):
    return call(
        half_kernel,
        jax.ShapeDtypeStruct((128, 1024), bf16),
        (*pieces,),
        [WHOLE] * len(pieces),
        flops=20 * 128 * 1024,
        moved=3 << 20,
    )


def square_kernel(*refs):
    lefts, rights, outs, right = refs[:4], refs[4:12], refs[12:16], refs[16]
    left, sems = refs[17:]
    x, y, core, zlo, zhi = position()
    z = zhi * 2 + zlo
    copies = []
    for k, (ref, step) in enumerate(zip(lefts, (0, *STEPS))):
        slot = lax.rem(y - step - x + 8, 4)
        copies.append(
            pltpu.make_async_copy(
                ref, left.at[pl.ds(pl.multiple_of(slot * 128, 128), 128)], sems.at[k]
            )
        )
    for k, ref in enumerate(rights):
        slot = (k // 4) * 4 + lax.rem(z - (0, *STEPS)[k % 4] + 4, 4)
        copies.append(
            pltpu.make_async_copy(
                ref, right.at[pl.ds(pl.multiple_of(slot * 128, 128), 128)], sems.at[4 + k]
            )
        )
    for copy in copies:
        copy.start()
    for copy in copies:
        copy.wait()
    product = lax.dot_general(
        left[...], right[...], (((1,), (1,)), ((), ())), preferred_element_type=f32
    )
    meets = (lax.rem(x, 2) == lax.div(y, 2)).astype(f32)
    for slot in range(8):
        of_core = core if slot < 4 else 1 - core
        scale = meets * (lax.div(x, 2) == slot % 2).astype(f32)
        at = slot % 4 // 2 * 512 + of_core * 256 + lax.rem(y, 2) * 128
        term = left[:, pl.ds(pl.multiple_of(at, 128), 128)].astype(f32)
        cols = slice(slot * 128, (slot + 1) * 128)
        value = (product[:, cols] - scale * term).astype(bf16)
        for k, out in enumerate(outs):
            out[:, cols] = value[k * 128 : (k + 1) * 128]


def square_pieces(lefts, rights):
    out = jax.ShapeDtypeStruct((128, 1024), bf16)
    return call(
        square_kernel,
        (out,) * 4 + (jax.ShapeDtypeStruct((1024, 1024), bf16),),
        (*lefts, *rights),
        [ANYWHERE] * 12,
        scratch=[
            pltpu.VMEM((512, 1024), bf16),
            pltpu.SemaphoreType.DMA((12,)),
        ],
        flops=2 * 512 * 1024 * 1024,
        moved=4 << 20,
    )


def factor_kernel(right, out, staged, sems):
    x, y, core, _, _ = position()
    row = lax.broadcasted_iota(jnp.int32, (128, 1024), 0)
    col = lax.broadcasted_iota(jnp.int32, (128, 1024), 1)
    copies = []
    for k in range(8):
        of_core = core if k < 4 else 1 - core
        block = k % 2 * 16 + lax.div(y, 2) * 8 + k % 4 // 2 * 4 + of_core * 2 + lax.rem(y, 2)
        diagonal = row + (block * 128 - x * 1024) == col
        rows = slice(k * 128, (k + 1) * 128)
        staged[rows] = (jnp.where(diagonal, 1.0, 0.0) - right[rows].astype(f32)).astype(bf16)
        copies.append(pltpu.make_async_copy(staged.at[rows], out.at[rows], sems.at[k]))
        copies[-1].start()
    for copy in copies:
        copy.wait()


def factor_of(right):
    return call(
        factor_kernel,
        pltpu.HBM((1024, 1024), bf16),
        (right,),
        [WHOLE],
        scratch=[pltpu.VMEM((1024, 1024), bf16), pltpu.SemaphoreType.DMA((8,))],
        flops=4 * 1024 * 1024,
        moved=4 << 20,
        to=pl.BlockSpec(memory_space=pltpu.HBM),
    )


def mix_kernel(*refs):
    pieces, out, staged, sems = refs[:4], refs[4], refs[5], refs[6]
    x, y, _, zlo, zhi = position()
    total = pieces[0][...].astype(f32)
    for ref in pieces[1:]:
        total += ref[...].astype(f32)
    row = lax.broadcasted_iota(jnp.int32, (128, 1024), 0)
    col = lax.broadcasted_iota(jnp.int32, (128, 1024), 1)
    first = jnp.where(x == y, (zhi * 2 + zlo) * 128, 4096)
    total = (total + jnp.where(row + first == col, 1.0, 0.0)).astype(bf16)
    for part in range(4):
        staged[part % 2, part // 2 * 32 : part // 2 * 32 + 32] = total[part * 32 : part * 32 + 32]
    copies = []
    for to_x in range(4):
        copies.append(
            pltpu.make_async_copy(staged, out.at[pl.ds(to_x * 2, 2)], sems.at[to_x])
        )
        copies[-1].start()
    for copy in copies:
        copy.wait()


def mixed(pieces):
    return call(
        mix_kernel,
        pltpu.HBM((8, 64, 1024), bf16),
        (*pieces,),
        [WHOLE] * 4,
        scratch=[pltpu.VMEM((2, 64, 1024), bf16), pltpu.SemaphoreType.DMA((4,))],
        to=pl.BlockSpec(memory_space=pltpu.HBM),
        flops=8 * 128 * 1024,
        moved=2 << 20,
    )


def cube_kernel(squares_in, factor_in, *refs):
    outs = refs[:4]
    factor, total, squares, sems = refs[4:]
    _, y, _, _, _ = position()
    copies = [
        pltpu.make_async_copy(squares_in, squares, sems.at[0]),
        pltpu.make_async_copy(factor_in, factor, sems.at[1]),
    ]
    for copy in copies:
        copy.start()
    for copy in copies:
        copy.wait()
    total[...] = jnp.dot(squares[...], factor[...], preferred_element_type=f32)
    for k, out in enumerate(outs):
        to_y = lax.rem(y + k, 4)
        for f7 in range(2):
            at = ((lax.div(to_y, 2) * 2 + f7) * 2 + lax.rem(to_y, 2)) * 64
            out[f7 * 64 : (f7 + 1) * 64] = total[pl.ds(pl.multiple_of(at, 64), 64)].astype(bf16)


def cube_pieces(squares, factor):
    out = jax.ShapeDtypeStruct((128, 1024), bf16)
    return call(
        cube_kernel,
        (out,) * 4,
        (squares, factor),
        [ANYWHERE, pl.BlockSpec(memory_space=pltpu.HBM)],
        scratch=[
            pltpu.VMEM((1024, 1024), bf16),
            pltpu.VMEM((512, 1024), f32),
            pltpu.VMEM((512, 1024), bf16),
            pltpu.SemaphoreType.DMA((2,)),
        ],
        flops=2 * 512 * 1024 * 1024,
        moved=4 << 20,
    )


def cut_kernel(*refs):
    pieces, outs = refs[:4], refs[4:]
    x = lax.axis_index("x")
    for k, out in enumerate(outs):
        rows = pl.ds(pl.multiple_of(lax.rem(x + k, 4) * 32, 32), 32)
        total = pieces[0][rows].astype(f32)
        for ref in pieces[1:]:
            total += ref[rows].astype(f32)
        out[...] = total.astype(bf16)


def cut(pieces):
    out = jax.ShapeDtypeStruct((32, 1024), bf16)
    return call(
        cut_kernel, (out,) * 4, (*pieces,), [WHOLE] * 4, flops=4 * 128 * 1024, moved=2 << 20
    )


def out_kernel(*refs):
    pieces, out = refs[:4], refs[4]
    x, y, core, zlo, zhi = position()
    first = (((zlo * 4 + y) * 2 + core) * 8 + x * 2 + zhi) * 32
    row = lax.broadcasted_iota(jnp.int32, (32, 1024), 0)
    col = lax.broadcasted_iota(jnp.int32, (32, 1024), 1)
    for k, ref in enumerate(pieces):
        source = lax.rem(x - k + 4, 4)
        diagonal = row + (first - source * 1024) == col
        out[:, pl.ds(pl.multiple_of(source * 1024, 1024), 1024)] = ref[...].astype(
            f32
        ) + jnp.where(diagonal, P0 - 1.0, 0.0)


def assembled(pieces):
    return call(
        out_kernel,
        jax.ShapeDtypeStruct((32, D), f32),
        (*pieces,),
        [WHOLE] * 4,
        flops=2 * 32 * D,
        moved=1 << 20,
    )


def body(activations, out_grads):
    zlo, y, core = (lax.axis_index(a) for a in TOK)
    x, zhi = (lax.axis_index(a) for a in BLK)
    both = (activations, out_grads)

    results = []
    for n, data in enumerate(both):
        shards = from_ring(data.T, "x")
        away = other_zhi(data)
        sent = gram_half(False, False, shards, data, away)
        received = other_core(sent)
        pair = gram_half(True, n == 1, shards, data, away, (received,))
        if n == 1:
            pieces = [pair[0]] + [to_y_and_zlo(pair[k], k % 4, k // 4) for k in range(1, 8)]
        else:
            pieces = (exchange(pair.reshape(8, 136, 1024), ("zlo", "y")),)
        half = halves(pieces)
        mine = from_ring(half, Z)
        lefts = from_ring(half, "y")
        rights = mine + [other_core(piece) for piece in mine]
        *parts, right = square_pieces(lefts, rights)
        factor = factor_of(right)
        parts = along_ring(parts, "x")
        square = mixed(parts)
        square = exchange(square, BLK).reshape(512, 1024)
        parts = cube_pieces(square, factor)
        parts = along_ring(parts, "y")
        parts = cut(parts)
        parts = along_ring(parts, "x")
        results.append(assembled(parts))
    return tuple(results)


def solution(mesh):
    split = Mesh(mesh.devices.reshape(2, 4, 2, 4, 2), NAMES)
    placed = P(TOK, BLK)
    return jax.shard_map(
        body,
        mesh=split,
        in_specs=(placed, placed),
        out_specs=(P(NAMES, None), P(NAMES, None)),
        check_vma=False,
    )
```

```python
import functools

import jax
import jax.numpy as jnp
from jax import lax
from jax.experimental import pallas as pl
from jax.experimental.pallas import tpu as pltpu
from jax.sharding import Mesh, PartitionSpec as P


D = 4096
TOKENS = 8192
damping = 0.3
epsilon = 1e-06
divisor = 2.0

CENTER = 2.0 / 3.0
P0 = 4.0 - 6.0 * CENTER + 4.0 * CENTER**2 - CENTER**3

NAMES = ("zlo", "y", "core", "x", "zhi")
TOK = ("zlo", "y", "core")
BLK = ("x", "zhi")
Z = ("zlo", "zhi")
STEPS = (1, -1, 2)
f32 = jnp.float32
bf16 = jnp.bfloat16
WHOLE = pl.BlockSpec(memory_space=pltpu.VMEM)
ANYWHERE = pl.BlockSpec(memory_space=pl.ANY)


def exchange(pieces, axes):
    return lax.all_to_all(pieces, axes, 0, 0, tiled=True)


def shifted_by(value, axis, step):
    place = (lambda z: (z % 2) * 2 + z // 2) if axis == Z else (lambda i: i)
    return lax.ppermute(value, axis, [(place(i), place((i + step) % 4)) for i in range(4)])


def to_y_and_zlo(value, step, flip):
    pairs = [
        (zlo * 4 + y, (zlo ^ flip) * 4 + (y + step) % 4) for zlo in range(2) for y in range(4)
    ]
    return lax.ppermute(value, ("zlo", "y"), pairs)


def from_ring(value, axis):
    return [value] + [shifted_by(value, axis, step) for step in STEPS]


def along_ring(pieces, axis):
    return [pieces[0]] + [shifted_by(pieces[k], axis, k) for k in range(1, 4)]


def other_core(value):
    return lax.ppermute(value, "core", [(0, 1), (1, 0)])


def other_zhi(value):
    return lax.ppermute(value, "zhi", [(0, 1), (1, 0)])


def position():
    return [lax.axis_index(a) for a in ("x", "y", "core", "zlo", "zhi")]


def call(kernel, outs, operands, specs, scratch=(), flops=0, moved=0, to=WHOLE):
    return pl.pallas_call(
        kernel,
        out_shape=outs,
        in_specs=specs,
        out_specs=jax.tree.map(lambda _: to, outs),
        scratch_shapes=list(scratch),
        compiler_params=pltpu.CompilerParams(vmem_limit_bytes=12 * 1024 * 1024),
        cost_estimate=pl.CostEstimate(flops=flops, bytes_accessed=moved, transcendentals=0),
    )(*operands)


def three_parts(value):
    high = value.astype(bf16).astype(f32)
    rest = value - high
    middle = rest.astype(bf16).astype(f32)
    return high, middle, rest - middle


def sum_rows(of_cols, of_rows):
    row = lax.broadcasted_iota(jnp.int32, (8, 1024), 0)
    of_rows = jnp.concatenate([of_rows, jnp.zeros((1, 896), f32)], axis=1)
    packed = jnp.zeros((8, 1024), f32)
    for k, part in enumerate((*three_parts(of_cols), *three_parts(of_rows))):
        packed = jnp.where(row == k, part, packed)
    return packed.astype(bf16)


def gram_kernel(keep, apart, *refs):
    shards, own, other = refs[:8], refs[8], refs[9]
    received = refs[10] if keep else None
    outs = refs[10 + keep : -5]
    b, a, added, staged, sems = refs[-5:]
    x, y, core, zlo, zhi = position()
    which = core if keep else 1 - core
    copies = [
        pltpu.make_async_copy(own, a.at[zhi], sems.at[4]),
        pltpu.make_async_copy(other, a.at[1 - zhi], sems.at[5]),
    ]
    stores = []
    for copy in copies:
        copy.start()
    for k, step in enumerate((0, *STEPS)):
        for part in range(2):

            @pl.when(which == part)
            def _():
                pltpu.make_async_copy(shards[2 * k + part], b.at[k], sems.at[k]).start()

        if keep:
            source = lax.rem(x - step + 4, 4)
            pltpu.make_async_copy(received.at[source], added.at[k], sems.at[10 + k]).start()
    for copy in copies:
        copy.wait()
    of_cols = jnp.concatenate(
        [jnp.sum(jnp.square(a[h].astype(f32)), axis=0, keepdims=True) for h in range(2)], axis=1
    )

    def one_shard(k, carry):
        source = lax.rem(x - jnp.where(k == 2, 3, jnp.where(k == 3, 2, k)) + 4, 4)
        pltpu.make_async_copy(shards[0], b.at[k], sems.at[k]).wait()
        if keep:
            pltpu.make_async_copy(received.at[source], added.at[k], sems.at[10 + k]).wait()
        for half in range(2):
            cols = slice(half * 512, (half + 1) * 512)
            piece = jnp.dot(b[k], a[half], preferred_element_type=f32).astype(bf16)
            for part in range(2):
                value = piece[part * 128 : (part + 1) * 128]
                if keep:
                    value = value.astype(f32) + added[k, part, :128, cols].astype(f32)
                staged[source, part, :128, cols] = value.astype(bf16)
        squares = jnp.square(b[k].astype(f32))
        squares = sum(squares[:, q * 128 : (q + 1) * 128] for q in range(4))
        for part in range(2):
            of_rows = jnp.sum(squares[part * 128 : (part + 1) * 128].T, axis=0, keepdims=True)
            cols = of_cols
            if keep:
                more = added[k, part, 128:136].astype(f32)
                cols = cols + more[0:1] + more[1:2] + more[2:3]
                of_rows = of_rows + (more[3:4] + more[4:5] + more[5:6])[:, :128]
            staged[source, part, 128:136] = sum_rows(cols, of_rows)
        if not apart:
            pltpu.make_async_copy(staged.at[source], outs[0].at[source], sems.at[6 + k]).start()
        return carry

    lax.fori_loop(0, 4, one_shard, 0)
    if not apart:
        for k in range(4):
            stores.append(pltpu.make_async_copy(staged.at[k], outs[0].at[k], sems.at[6 + k]))
    if apart:
        for k, out in enumerate(outs):
            to_y = lax.rem(y + k % 4, 4)
            to_zlo = zlo if k < 4 else 1 - zlo
            piece = staged.at[to_zlo * 2 + lax.div(to_y, 2), lax.rem(to_y, 2)]
            stores.append(pltpu.make_async_copy(piece, out, sems.at[14 + k]))
            stores[-1].start()
    for copy in stores:
        copy.wait()


def gram_half(keep, apart, shards, own, other, received=()):
    shape = (4, 2, 136, 1024)
    if apart:
        out = (pltpu.HBM((136, 1024), bf16),) + (jax.ShapeDtypeStruct((136, 1024), bf16),) * 7
    else:
        out = pltpu.HBM(shape, bf16) if keep else jax.ShapeDtypeStruct(shape, bf16)
    return call(
        functools.partial(gram_kernel, keep, apart),
        out,
        (*shards, own, other, *received),
        [ANYWHERE] * (10 + keep),
        scratch=[
            pltpu.VMEM((4, 256, 512), bf16),
            pltpu.VMEM((2, 512, 512), bf16),
            pltpu.VMEM(shape if keep else (8, 128), bf16),
            pltpu.VMEM(shape, bf16),
            pltpu.SemaphoreType.DMA((22,)),
        ],
        to=ANYWHERE if apart else pl.BlockSpec(memory_space=pltpu.HBM),
        flops=512 * 1024 * 2048,
        moved=7 << 20,
    )


def turn_kernel(data, top, bottom):
    for k, out in enumerate((top, bottom)):
        out[...] = data[:, k * 256 : (k + 1) * 256].T


def turned(data):
    out = jax.ShapeDtypeStruct((256, 512), bf16)
    return call(turn_kernel, (out, out), (data,), [WHOLE], flops=512 * 512, moved=1 << 20)


def half_kernel(*refs):
    half = refs[-1]
    pieces = refs[:-1] if len(refs) > 2 else [refs[0].at[k] for k in range(8)]
    x, y, core, zlo, zhi = position()
    block = zlo * 16 + lax.div(y, 2) * 8 + zhi * 4 + core * 2 + lax.rem(y, 2)
    sums = pieces[0][128:136].astype(f32)
    for k in range(1, 8):
        sums += pieces[k][128:136].astype(f32)
    by_col = lax.rsqrt((sums[0:1] + sums[1:2] + sums[2:3]) / TOKENS + epsilon)
    by_row = lax.rsqrt((sums[3:4] + sums[4:5] + sums[5:6])[:, :128] / TOKENS + epsilon)
    by_row = (jnp.broadcast_to(by_row, (128, 128)) / (TOKENS * divisor)).T[:, :1]
    for part in range(4):
        rows = slice(part * 32, part * 32 + 32)
        row = lax.broadcasted_iota(jnp.int32, (32, 1024), 0) + part * 32
        col = lax.broadcasted_iota(jnp.int32, (32, 1024), 1)
        diagonal = row + (block * 128 - x * 1024) == col
        gram = pieces[0][rows].astype(f32)
        for k in range(1, 8):
            gram += pieces[k][rows].astype(f32)
        value = gram * by_row[rows] * by_col
        value += jnp.where(diagonal, damping / divisor - CENTER, 0.0)
        value = value.astype(bf16)
        half[rows] = value


def halves(pieces):
    return call(
        half_kernel,
        jax.ShapeDtypeStruct((128, 1024), bf16),
        (*pieces,),
        [WHOLE] * len(pieces),
        flops=20 * 128 * 1024,
        moved=3 << 20,
    )


def square_kernel(*refs):
    lefts, rights, outs, right = refs[:4], refs[4:12], refs[12:16], refs[16]
    left, sems = refs[17:]
    x, y, core, zlo, zhi = position()
    z = zhi * 2 + zlo
    copies = []
    for k, (ref, step) in enumerate(zip(lefts, (0, *STEPS))):
        slot = lax.rem(y - step - x + 8, 4)
        copies.append(
            pltpu.make_async_copy(
                ref, left.at[pl.ds(pl.multiple_of(slot * 128, 128), 128)], sems.at[k]
            )
        )
    for k, ref in enumerate(rights):
        slot = (k // 4) * 4 + lax.rem(z - (0, *STEPS)[k % 4] + 4, 4)
        copies.append(
            pltpu.make_async_copy(
                ref, right.at[pl.ds(pl.multiple_of(slot * 128, 128), 128)], sems.at[4 + k]
            )
        )
    for copy in copies:
        copy.start()
    for copy in copies:
        copy.wait()
    product = lax.dot_general(
        left[...], right[...], (((1,), (1,)), ((), ())), preferred_element_type=f32
    )
    meets = (lax.rem(x, 2) == lax.div(y, 2)).astype(f32)
    for slot in range(8):
        of_core = core if slot < 4 else 1 - core
        scale = meets * (lax.div(x, 2) == slot % 2).astype(f32)
        at = slot % 4 // 2 * 512 + of_core * 256 + lax.rem(y, 2) * 128
        term = left[:, pl.ds(pl.multiple_of(at, 128), 128)].astype(f32)
        cols = slice(slot * 128, (slot + 1) * 128)
        value = (product[:, cols] - scale * term).astype(bf16)
        for k, out in enumerate(outs):
            out[:, cols] = value[k * 128 : (k + 1) * 128]


def square_pieces(lefts, rights):
    out = jax.ShapeDtypeStruct((128, 1024), bf16)
    return call(
        square_kernel,
        (out,) * 4 + (jax.ShapeDtypeStruct((1024, 1024), bf16),),
        (*lefts, *rights),
        [ANYWHERE] * 12,
        scratch=[
            pltpu.VMEM((512, 1024), bf16),
            pltpu.SemaphoreType.DMA((12,)),
        ],
        flops=2 * 512 * 1024 * 1024,
        moved=4 << 20,
    )


def factor_kernel(right, out, staged, sems):
    x, y, core, _, _ = position()
    row = lax.broadcasted_iota(jnp.int32, (128, 1024), 0)
    col = lax.broadcasted_iota(jnp.int32, (128, 1024), 1)
    copies = []
    for k in range(8):
        of_core = core if k < 4 else 1 - core
        block = k % 2 * 16 + lax.div(y, 2) * 8 + k % 4 // 2 * 4 + of_core * 2 + lax.rem(y, 2)
        diagonal = row + (block * 128 - x * 1024) == col
        rows = slice(k * 128, (k + 1) * 128)
        staged[rows] = (jnp.where(diagonal, 1.0, 0.0) - right[rows].astype(f32)).astype(bf16)
        copies.append(pltpu.make_async_copy(staged.at[rows], out.at[rows], sems.at[k]))
        copies[-1].start()
    for copy in copies:
        copy.wait()


def factor_of(right):
    return call(
        factor_kernel,
        pltpu.HBM((1024, 1024), bf16),
        (right,),
        [WHOLE],
        scratch=[pltpu.VMEM((1024, 1024), bf16), pltpu.SemaphoreType.DMA((8,))],
        flops=4 * 1024 * 1024,
        moved=4 << 20,
        to=ANYWHERE,
    )


def mix_kernel(*refs):
    pieces, outs = refs[:4], refs[4:]
    x, y, _, zlo, zhi = position()
    row = lax.broadcasted_iota(jnp.int32, (32, 1024), 0)
    col = lax.broadcasted_iota(jnp.int32, (32, 1024), 1)
    first = jnp.where(x == y, (zhi * 2 + zlo) * 128, 4096)
    for away, out in enumerate(outs):
        f5 = 1 - zhi if away else zhi
        for f6 in range(2):
            at = f6 * 64 + f5 * 32
            rows = pl.ds(pl.multiple_of(at, 32), 32)
            total = pieces[0][rows].astype(f32)
            for ref in pieces[1:]:
                total += ref[rows].astype(f32)
            total += jnp.where(row + (first + at) == col, 1.0, 0.0)
            out[f6 * 32 : (f6 + 1) * 32] = total.astype(bf16)


def mixed(pieces):
    small = jax.ShapeDtypeStruct((64, 1024), bf16)
    return call(
        mix_kernel, (small, small), (*pieces,), [WHOLE] * 4, flops=8 * 128 * 1024, moved=2 << 20
    )


def pair_kernel(own, other, out):
    zhi = lax.axis_index("zhi")
    out[pl.ds(pl.multiple_of(zhi * 64, 64), 64)] = own[...]
    out[pl.ds(pl.multiple_of((1 - zhi) * 64, 64), 64)] = other[...]


def paired(own, other):
    return call(
        pair_kernel,
        jax.ShapeDtypeStruct((128, 1024), bf16),
        (own, other),
        [WHOLE] * 2,
        flops=128 * 1024,
        moved=1 << 19,
    )


def cube_kernel(*refs):
    squares_in, factor_in, outs = refs[:-9], refs[-9], refs[-8:-4]
    factor, total, squares, sems = refs[-4:]
    x, y, _, _, zhi = position()
    copies = [pltpu.make_async_copy(factor_in, factor, sems.at[8])]
    for k, ref in enumerate(squares_in):
        at = lax.rem(x - (0, *STEPS)[k % 4] + 4, 4) * 128
        if len(squares_in) == 8:
            at += 64 * (zhi if k < 4 else 1 - zhi)
        at = pl.ds(pl.multiple_of(at, 64), ref.shape[0])
        copies.append(pltpu.make_async_copy(ref, squares.at[at], sems.at[k]))
    for copy in copies:
        copy.start()
    for copy in copies:
        copy.wait()
    total[...] = jnp.dot(squares[...], factor[...], preferred_element_type=f32)
    for k, out in enumerate(outs):
        to_y = lax.rem(y + k, 4)
        for f7 in range(2):
            at = ((lax.div(to_y, 2) * 2 + f7) * 2 + lax.rem(to_y, 2)) * 64
            out[f7 * 64 : (f7 + 1) * 64] = total[pl.ds(pl.multiple_of(at, 64), 64)].astype(bf16)


def cube_pieces(squares, factor):
    out = jax.ShapeDtypeStruct((128, 1024), bf16)
    return call(
        cube_kernel,
        (out,) * 4,
        (*squares, factor),
        [ANYWHERE] * (len(squares) + 1),
        scratch=[
            pltpu.VMEM((1024, 1024), bf16),
            pltpu.VMEM((512, 1024), f32),
            pltpu.VMEM((512, 1024), bf16),
            pltpu.SemaphoreType.DMA((9,)),
        ],
        flops=2 * 512 * 1024 * 1024,
        moved=4 << 20,
    )


def cut_kernel(*refs):
    pieces, outs = refs[:4], refs[4:]
    x = lax.axis_index("x")
    for k, out in enumerate(outs):
        rows = pl.ds(pl.multiple_of(lax.rem(x + k, 4) * 32, 32), 32)
        total = pieces[0][rows].astype(f32)
        for ref in pieces[1:]:
            total += ref[rows].astype(f32)
        out[...] = total.astype(bf16)


def cut(pieces):
    out = jax.ShapeDtypeStruct((32, 1024), bf16)
    return call(
        cut_kernel, (out,) * 4, (*pieces,), [WHOLE] * 4, flops=4 * 128 * 1024, moved=2 << 20
    )


def out_kernel(*refs):
    pieces, out = refs[:4], refs[4]
    x, y, core, zlo, zhi = position()
    first = (((zlo * 4 + y) * 2 + core) * 8 + x * 2 + zhi) * 32
    row = lax.broadcasted_iota(jnp.int32, (32, 1024), 0)
    col = lax.broadcasted_iota(jnp.int32, (32, 1024), 1)
    for k, ref in enumerate(pieces):
        source = lax.rem(x - k + 4, 4)
        diagonal = row + (first - source * 1024) == col
        out[:, pl.ds(pl.multiple_of(source * 1024, 1024), 1024)] = ref[...].astype(
            f32
        ) + jnp.where(diagonal, P0 - 1.0, 0.0)


def assembled(pieces):
    return call(
        out_kernel,
        jax.ShapeDtypeStruct((32, D), f32),
        (*pieces,),
        [WHOLE] * 4,
        flops=2 * 32 * D,
        moved=1 << 20,
    )


def body(activations, out_grads):
    zlo, y, core = (lax.axis_index(a) for a in TOK)
    x, zhi = (lax.axis_index(a) for a in BLK)
    both = (activations, out_grads)

    results = []
    for n, data in enumerate(both):
        own = turned(data)
        left_top = shifted_by(own[0], "x", 1)
        right_bottom = shifted_by(own[1], "x", -1)
        left_bottom = shifted_by(own[1], "x", 1)
        right_top = shifted_by(own[0], "x", -1)
        away = other_zhi(data)
        far_top = shifted_by(left_top, "x", 1)
        far_bottom = shifted_by(right_bottom, "x", -1)
        shards = (*own, left_top, left_bottom, right_top, right_bottom, far_top, far_bottom)
        sent = gram_half(False, False, shards, data, away)
        received = other_core(sent)
        pair = gram_half(True, n == 1, shards, data, away, (received,))
        if n == 1:
            pieces = [pair[0]] + [to_y_and_zlo(pair[k], k % 4, k // 4) for k in range(1, 8)]
        else:
            pieces = (exchange(pair.reshape(8, 136, 1024), ("zlo", "y")),)
        half = halves(pieces)
        mine = from_ring(half, Z)
        lefts = from_ring(half, "y")
        rights = mine + [other_core(piece) for piece in mine]
        *parts, right = square_pieces(lefts, rights)
        factor = factor_of(right)
        parts = along_ring(parts, "x")
        near, away = mixed(parts)
        other = other_zhi(away)
        if n == 0:
            square = paired(near, other)
            square = from_ring(square, "x")
        else:
            square = from_ring(near, "x")
            square += from_ring(other, "x")
        parts = cube_pieces(square, factor)
        parts = along_ring(parts, "y")
        parts = cut(parts)
        parts = along_ring(parts, "x")
        results.append(assembled(parts))
    return tuple(results)


def solution(mesh):
    split = Mesh(mesh.devices.reshape(2, 4, 2, 4, 2), NAMES)
    placed = P(TOK, BLK)
    return jax.shard_map(
        body,
        mesh=split,
        in_specs=(placed, placed),
        out_specs=(P(NAMES, None), P(NAMES, None)),
        check_vma=False,
    )
```

```python
import functools

import jax
import jax.numpy as jnp
from jax import lax
from jax.experimental import pallas as pl
from jax.experimental.pallas import tpu as pltpu
from jax.sharding import Mesh, PartitionSpec as P


D = 4096
TOKENS = 8192
damping = 0.3
epsilon = 1e-06
divisor = 2.0

CENTER = 2.0 / 3.0
P0 = 4.0 - 6.0 * CENTER + 4.0 * CENTER**2 - CENTER**3

NAMES = ("zlo", "y", "core", "x", "zhi")
TOK = ("zlo", "y", "core")
BLK = ("x", "zhi")
Z = ("zlo", "zhi")
STEPS = (1, -1, 2)
f32 = jnp.float32
bf16 = jnp.bfloat16
WHOLE = pl.BlockSpec(memory_space=pltpu.VMEM)
ANYWHERE = pl.BlockSpec(memory_space=pl.ANY)


def shifted_by(value, axis, step):
    place = (lambda z: (z % 2) * 2 + z // 2) if axis == Z else (lambda i: i)
    return lax.ppermute(value, axis, [(place(i), place((i + step) % 4)) for i in range(4)])


def from_ring(value, axis):
    return [value] + [shifted_by(value, axis, step) for step in STEPS]


def along_ring(pieces, axis):
    return [pieces[0]] + [shifted_by(pieces[k], axis, k) for k in range(1, 4)]


def other_core(value):
    return lax.ppermute(value, "core", [(0, 1), (1, 0)])


def other_zlo(value):
    return lax.ppermute(value, "zlo", [(0, 1), (1, 0)])


def other_zhi(value):
    return lax.ppermute(value, "zhi", [(0, 1), (1, 0)])


def position():
    return [lax.axis_index(a) for a in ("x", "y", "core", "zlo", "zhi")]


def call(kernel, outs, operands, specs, scratch=(), flops=0, moved=0, to=WHOLE):
    return pl.pallas_call(
        kernel,
        out_shape=outs,
        in_specs=specs,
        out_specs=jax.tree.map(lambda _: to, outs),
        scratch_shapes=list(scratch),
        compiler_params=pltpu.CompilerParams(vmem_limit_bytes=12 * 1024 * 1024),
        cost_estimate=pl.CostEstimate(flops=flops, bytes_accessed=moved, transcendentals=0),
    )(*operands)


def three_parts(value):
    high = value.astype(bf16).astype(f32)
    rest = value - high
    middle = rest.astype(bf16).astype(f32)
    return high, middle, rest - middle


def sum_rows(of_cols, of_rows):
    row = lax.broadcasted_iota(jnp.int32, (8, 1024), 0)
    of_rows = jnp.concatenate([of_rows, jnp.zeros((1, 896), f32)], axis=1)
    packed = jnp.zeros((8, 1024), f32)
    for k, part in enumerate((*three_parts(of_cols), *three_parts(of_rows))):
        packed = jnp.where(row == k, part, packed)
    return packed.astype(bf16)


def gram_kernel(keep, apart, *refs):
    shards, own, other = refs[:8], refs[8], refs[9]
    received = refs[10] if keep else None
    outs = refs[10 + keep : -5]
    b, a, added, staged, sems = refs[-5:]
    x, y, core, _, zhi = position()
    which = core if keep else 1 - core
    copies = [
        pltpu.make_async_copy(own, a.at[zhi], sems.at[4]),
        pltpu.make_async_copy(other, a.at[1 - zhi], sems.at[5]),
    ]
    stores = []
    for copy in copies:
        copy.start()
    for k, step in enumerate((0, *STEPS)):
        for part in range(2):

            @pl.when(which == part)
            def _():
                pltpu.make_async_copy(shards[2 * k + part], b.at[k], sems.at[k]).start()

        if keep:
            source = lax.rem(x - step + 4, 4)
            pltpu.make_async_copy(received.at[source], added.at[k], sems.at[10 + k]).start()
    for copy in copies:
        copy.wait()
    of_cols = jnp.concatenate(
        [jnp.sum(jnp.square(a[h].astype(f32)), axis=0, keepdims=True) for h in range(2)], axis=1
    )

    def one_shard(k, carry):
        source = lax.rem(x - jnp.where(k == 2, 3, jnp.where(k == 3, 2, k)) + 4, 4)
        pltpu.make_async_copy(shards[0], b.at[k], sems.at[k]).wait()
        if keep:
            pltpu.make_async_copy(received.at[source], added.at[k], sems.at[10 + k]).wait()
        for half in range(2):
            cols = slice(half * 512, (half + 1) * 512)
            piece = jnp.dot(b[k], a[half], preferred_element_type=f32).astype(bf16)
            for part in range(2):
                value = piece[part * 128 : (part + 1) * 128]
                if keep:
                    value = value.astype(f32) + added[k, part, :128, cols].astype(f32)
                staged[source, part, :128, cols] = value.astype(bf16)
        squares = jnp.square(b[k].astype(f32))
        squares = sum(squares[:, q * 128 : (q + 1) * 128] for q in range(4))
        for part in range(2):
            of_rows = jnp.sum(squares[part * 128 : (part + 1) * 128].T, axis=0, keepdims=True)
            cols = of_cols
            if keep:
                more = added[k, part, 128:136].astype(f32)
                cols = cols + more[0:1] + more[1:2] + more[2:3]
                of_rows = of_rows + (more[3:4] + more[4:5] + more[5:6])[:, :128]
            staged[source, part, 128:136] = sum_rows(cols, of_rows)
        if not apart:
            pltpu.make_async_copy(staged.at[source], outs[0].at[source], sems.at[6 + k]).start()
        return carry

    lax.fori_loop(0, 4, one_shard, 0)
    if not apart:
        for k in range(4):
            stores.append(pltpu.make_async_copy(staged.at[k], outs[0].at[k], sems.at[6 + k]))
    if apart:
        for k, out in enumerate(outs):
            to_y = lax.rem(y + k // 2, 4)
            piece = staged.at[k % 2 * 2 + lax.div(to_y, 2), lax.rem(to_y, 2)]
            stores.append(pltpu.make_async_copy(piece, out, sems.at[14 + k]))
            stores[-1].start()
    for copy in stores:
        copy.wait()


def gram_half(keep, apart, shards, own, other, received=()):
    shape = (4, 2, 136, 1024)
    if apart:
        out = (jax.ShapeDtypeStruct((136, 1024), bf16),) * 8
    else:
        out = jax.ShapeDtypeStruct(shape, bf16)
    return call(
        functools.partial(gram_kernel, keep, apart),
        out,
        (*shards, own, other, *received),
        [ANYWHERE] * (10 + keep),
        scratch=[
            pltpu.VMEM((4, 256, 512), bf16),
            pltpu.VMEM((2, 512, 512), bf16),
            pltpu.VMEM(shape if keep else (8, 128), bf16),
            pltpu.VMEM(shape, bf16),
            pltpu.SemaphoreType.DMA((22,)),
        ],
        to=ANYWHERE,
        flops=512 * 1024 * 2048,
        moved=7 << 20,
    )


def turn_kernel(data, top, bottom):
    for k, out in enumerate((top, bottom)):
        out[...] = data[:, k * 256 : (k + 1) * 256].T


def turned(data):
    out = jax.ShapeDtypeStruct((256, 512), bf16)
    return call(turn_kernel, (out, out), (data,), [WHOLE], flops=512 * 512, moved=1 << 20)


def add_up(refs, out):
    def some_rows(k, carry):
        rows = pl.ds(pl.multiple_of(k * 32, 32), 32)
        total = refs[0][rows].astype(f32)
        for ref in refs[1:]:
            total += ref[rows].astype(f32)
        out[rows] = total.astype(bf16)
        return carry

    lax.fori_loop(0, 4, some_rows, 0)
    sums = refs[0][128:136].astype(f32)
    for ref in refs[1:]:
        sums += ref[128:136].astype(f32)
    of_cols = sums[0:1] + sums[1:2] + sums[2:3]
    of_rows = (sums[3:4] + sums[4:5] + sums[5:6])[:, :128]
    out[128:136] = sum_rows(of_cols, of_rows)


def relay_kernel(*refs):
    for k, out in enumerate(refs[4:6]):
        add_up(refs[2 * k : 2 * k + 2], out)


def y_sum_kernel(*refs):
    keep, send, staged, sems = refs[6:]
    zlo = lax.axis_index("zlo")
    for k in range(2):
        add_up(refs[3 * k : 3 * k + 3], staged.at[k])
    copies = [
        pltpu.make_async_copy(staged.at[zlo], keep, sems.at[0]),
        pltpu.make_async_copy(staged.at[1 - zlo], send, sems.at[1]),
    ]
    for copy in copies:
        copy.start()
    for copy in copies:
        copy.wait()


def piece_sums(kernel, pieces, scratch=()):
    out = jax.ShapeDtypeStruct((136, 1024), bf16)
    return call(
        kernel,
        (out, out),
        (*pieces,),
        [WHOLE] * len(pieces),
        scratch=scratch,
        to=ANYWHERE if scratch else WHOLE,
        flops=8 * 136 * 1024,
        moved=2 << 20,
    )


def half_kernel(*refs):
    pieces, half, scale = refs[:-2], refs[-2], refs[-1]
    x, y, core, zlo, zhi = position()
    block = zlo * 16 + lax.div(y, 2) * 8 + zhi * 4 + core * 2 + lax.rem(y, 2)
    sums = pieces[0][128:136].astype(f32)
    for ref in pieces[1:]:
        sums += ref[128:136].astype(f32)
    by_col = lax.rsqrt((sums[0:1] + sums[1:2] + sums[2:3]) / TOKENS + epsilon)
    by_row = lax.rsqrt((sums[3:4] + sums[4:5] + sums[5:6])[:, :128] / TOKENS + epsilon)
    by_row = (jnp.broadcast_to(by_row, (128, 128)) / (TOKENS * divisor)).T
    scale[...] = by_row

    def some_rows(k, carry):
        rows = pl.ds(pl.multiple_of(k * 32, 32), 32)
        row = lax.broadcasted_iota(jnp.int32, (32, 1024), 0) + k * 32
        col = lax.broadcasted_iota(jnp.int32, (32, 1024), 1)
        diagonal = row + (block * 128 - x * 1024) == col
        gram = pieces[0][rows].astype(f32)
        for ref in pieces[1:]:
            gram += ref[rows].astype(f32)
        value = gram * scale[rows, :1] * by_col
        value += jnp.where(diagonal, damping / divisor - CENTER, 0.0)
        half[rows] = value.astype(bf16)
        return carry

    lax.fori_loop(0, 4, some_rows, 0)


def halves(pieces):
    return call(
        half_kernel,
        jax.ShapeDtypeStruct((128, 1024), bf16),
        (*pieces,),
        [WHOLE] * len(pieces),
        scratch=[pltpu.VMEM((128, 128), f32)],
        flops=20 * 128 * 1024,
        moved=3 << 20,
    )


def square_kernel(*refs):
    lefts, rights, outs, right = refs[:4], refs[4:12], refs[12:16], refs[16]
    left, sems = refs[17:]
    x, y, core, zlo, zhi = position()
    z = zhi * 2 + zlo
    copies = []
    for k, (ref, step) in enumerate(zip(lefts, (0, *STEPS))):
        slot = lax.rem(y - step - x + 8, 4)
        copies.append(
            pltpu.make_async_copy(
                ref, left.at[pl.ds(pl.multiple_of(slot * 128, 128), 128)], sems.at[k]
            )
        )
    for k, ref in enumerate(rights):
        slot = (k // 4) * 4 + lax.rem(z - (0, *STEPS)[k % 4] + 4, 4)
        copies.append(
            pltpu.make_async_copy(
                ref, right.at[pl.ds(pl.multiple_of(slot * 128, 128), 128)], sems.at[4 + k]
            )
        )
    for copy in copies:
        copy.start()
    for copy in copies:
        copy.wait()
    meets = (lax.rem(x, 2) == lax.div(y, 2)).astype(f32)

    def some_columns(n, carry):
        rows = pl.ds(pl.multiple_of(n * 256, 256), 256)
        product = lax.dot_general(
            left[...], right[rows], (((1,), (1,)), ((), ())), preferred_element_type=f32
        )
        of_core = jnp.where(n < 2, core, 1 - core)
        for of_zlo in range(2):
            scale = meets * (lax.div(x, 2) == of_zlo).astype(f32)
            at = lax.rem(n, 2) * 512 + of_core * 256 + lax.rem(y, 2) * 128
            term = left[:, pl.ds(pl.multiple_of(at, 128), 128)].astype(f32)
            value = product[:, of_zlo * 128 : (of_zlo + 1) * 128] - scale * term
            value = value.astype(bf16)
            cols = pl.ds(pl.multiple_of(n * 256 + of_zlo * 128, 128), 128)
            for k, out in enumerate(outs):
                out[:, cols] = value[k * 128 : (k + 1) * 128]
        return carry

    lax.fori_loop(0, 4, some_columns, 0)


def square_pieces(lefts, rights):
    out = jax.ShapeDtypeStruct((128, 1024), bf16)
    return call(
        square_kernel,
        (out,) * 4 + (jax.ShapeDtypeStruct((1024, 1024), bf16),),
        (*lefts, *rights),
        [ANYWHERE] * 12,
        scratch=[
            pltpu.VMEM((512, 1024), bf16),
            pltpu.SemaphoreType.DMA((12,)),
        ],
        flops=2 * 512 * 1024 * 1024,
        moved=4 << 20,
    )


def factor_kernel(right, out, staged, sems):
    x, y, core, _, _ = position()
    row = lax.broadcasted_iota(jnp.int32, (128, 1024), 0)
    col = lax.broadcasted_iota(jnp.int32, (128, 1024), 1)

    def one_block(k, carry):
        of_core = jnp.where(k < 4, core, 1 - core)
        of_z = lax.rem(k, 4)
        block = lax.rem(k, 2) * 16 + lax.div(y, 2) * 8 + lax.div(of_z, 2) * 4
        block += of_core * 2 + lax.rem(y, 2)
        diagonal = row + (block * 128 - x * 1024) == col
        rows = pl.ds(pl.multiple_of(k * 128, 128), 128)
        staged[rows] = (jnp.where(diagonal, 1.0, 0.0) - right[rows].astype(f32)).astype(bf16)
        pltpu.make_async_copy(staged.at[rows], out.at[rows], sems.at[k]).start()
        return carry

    lax.fori_loop(0, 8, one_block, 0)
    for k in range(8):
        rows = pl.ds(k * 128, 128)
        pltpu.make_async_copy(staged.at[rows], out.at[rows], sems.at[k]).wait()


def factor_of(right):
    return call(
        factor_kernel,
        pltpu.HBM((1024, 1024), bf16),
        (right,),
        [WHOLE],
        scratch=[pltpu.VMEM((1024, 1024), bf16), pltpu.SemaphoreType.DMA((8,))],
        flops=4 * 1024 * 1024,
        moved=4 << 20,
        to=ANYWHERE,
    )


def mix_kernel(*refs):
    pieces, outs = refs[:4], refs[4:]
    x, y, _, zlo, zhi = position()
    row = lax.broadcasted_iota(jnp.int32, (32, 1024), 0)
    col = lax.broadcasted_iota(jnp.int32, (32, 1024), 1)
    first = jnp.where(x == y, (zhi * 2 + zlo) * 128, 4096)
    for away, out in enumerate(outs):
        f5 = 1 - zhi if away else zhi
        for f6 in range(2):
            at = f6 * 64 + f5 * 32
            rows = pl.ds(pl.multiple_of(at, 32), 32)
            total = pieces[0][rows].astype(f32)
            for ref in pieces[1:]:
                total += ref[rows].astype(f32)
            total += jnp.where(row + (first + at) == col, 1.0, 0.0)
            out[f6 * 32 : (f6 + 1) * 32] = total.astype(bf16)


def mixed(pieces):
    small = jax.ShapeDtypeStruct((64, 1024), bf16)
    return call(
        mix_kernel, (small, small), (*pieces,), [WHOLE] * 4, flops=8 * 128 * 1024, moved=2 << 20
    )


def pair_kernel(own, other, out):
    zhi = lax.axis_index("zhi")
    out[pl.ds(pl.multiple_of(zhi * 64, 64), 64)] = own[...]
    out[pl.ds(pl.multiple_of((1 - zhi) * 64, 64), 64)] = other[...]


def paired(own, other):
    return call(
        pair_kernel,
        jax.ShapeDtypeStruct((128, 1024), bf16),
        (own, other),
        [WHOLE] * 2,
        flops=128 * 1024,
        moved=1 << 19,
    )


def cube_kernel(*refs):
    squares_in, factor_in, outs = refs[:-9], refs[-9], refs[-8:-4]
    factor, total, squares, sems = refs[-4:]
    x, y, _, _, zhi = position()
    copies = [pltpu.make_async_copy(factor_in, factor, sems.at[8])]
    for k, ref in enumerate(squares_in):
        at = lax.rem(x - (0, *STEPS)[k % 4] + 4, 4) * 128
        if len(squares_in) == 8:
            at += 64 * (zhi if k < 4 else 1 - zhi)
        at = pl.ds(pl.multiple_of(at, 64), ref.shape[0])
        copies.append(pltpu.make_async_copy(ref, squares.at[at], sems.at[k]))
    for copy in copies:
        copy.start()
    for copy in copies:
        copy.wait()

    def some_columns(n, carry):
        cols = pl.ds(pl.multiple_of(n * 256, 256), 256)
        total[:, cols] = jnp.dot(squares[...], factor[:, cols], preferred_element_type=f32)
        return carry

    lax.fori_loop(0, 4, some_columns, 0)
    for k, out in enumerate(outs):
        to_y = lax.rem(y + k, 4)
        for f7 in range(2):
            at = ((lax.div(to_y, 2) * 2 + f7) * 2 + lax.rem(to_y, 2)) * 64
            out[f7 * 64 : (f7 + 1) * 64] = total[pl.ds(pl.multiple_of(at, 64), 64)].astype(bf16)


def cube_pieces(squares, factor):
    out = jax.ShapeDtypeStruct((128, 1024), bf16)
    return call(
        cube_kernel,
        (out,) * 4,
        (*squares, factor),
        [ANYWHERE] * (len(squares) + 1),
        scratch=[
            pltpu.VMEM((1024, 1024), bf16),
            pltpu.VMEM((512, 1024), f32),
            pltpu.VMEM((512, 1024), bf16),
            pltpu.SemaphoreType.DMA((9,)),
        ],
        flops=2 * 512 * 1024 * 1024,
        moved=4 << 20,
    )


def cut_kernel(*refs):
    pieces, out, staged, sem = refs[:4], refs[4], refs[5], refs[6]
    for k in range(4):
        rows = slice(k * 32, (k + 1) * 32)
        total = pieces[0][rows].astype(f32)
        for ref in pieces[1:]:
            total += ref[rows].astype(f32)
        staged[k] = total.astype(bf16)
    copy = pltpu.make_async_copy(staged, out, sem)
    copy.start()
    copy.wait()


def cut(pieces):
    return call(
        cut_kernel,
        pltpu.HBM((4, 32, 1024), bf16),
        (*pieces,),
        [WHOLE] * 4,
        scratch=[pltpu.VMEM((4, 32, 1024), bf16), pltpu.SemaphoreType.DMA],
        to=pl.BlockSpec(memory_space=pltpu.HBM),
        flops=4 * 128 * 1024,
        moved=2 << 20,
    )


def out_kernel(pieces, out):
    x, y, core, zlo, zhi = position()
    first = (((zlo * 4 + y) * 2 + core) * 8 + x * 2 + zhi) * 32
    row = lax.broadcasted_iota(jnp.int32, (32, 1024), 0)
    col = lax.broadcasted_iota(jnp.int32, (32, 1024), 1)
    for k in range(4):
        diagonal = row + (first - k * 1024) == col
        out[:, k * 1024 : (k + 1) * 1024] = pieces[k].astype(f32) + jnp.where(
            diagonal, P0 - 1.0, 0.0
        )


def assembled(pieces):
    return call(
        out_kernel,
        jax.ShapeDtypeStruct((32, D), f32),
        (pieces,),
        [WHOLE],
        flops=2 * 32 * D,
        moved=1 << 20,
    )


def body(activations, out_grads):
    zlo, y, core = (lax.axis_index(a) for a in TOK)
    x, zhi = (lax.axis_index(a) for a in BLK)
    both = (activations, out_grads)

    results = []
    for n, data in enumerate(both):
        own = turned(data)
        left_top = shifted_by(own[0], "x", 1)
        right_bottom = shifted_by(own[1], "x", -1)
        left_bottom = shifted_by(own[1], "x", 1)
        right_top = shifted_by(own[0], "x", -1)
        away = other_zhi(data)
        far_top = shifted_by(left_top, "x", 1)
        far_bottom = shifted_by(right_bottom, "x", -1)
        shards = (*own, left_top, left_bottom, right_top, right_bottom, far_top, far_bottom)
        sent = gram_half(False, False, shards, data, away)
        received = other_core(sent)
        pieces = gram_half(True, True, shards, data, away, (received,))
        here, after, far, before = (pieces[2 * k : 2 * k + 2] for k in range(4))
        far_up = shifted_by(far[0], "y", 1)
        far_down = shifted_by(far[1], "y", -1)
        up_1 = shifted_by(after[1], "y", 1)
        down_0 = shifted_by(before[0], "y", -1)
        summed = (after[0], far_up, before[1], far_down)
        up_0, down_1 = piece_sums(relay_kernel, summed)
        up_0 = shifted_by(up_0, "y", 1)
        down_1 = shifted_by(down_1, "y", -1)
        summed = (here[0], up_0, down_0, here[1], up_1, down_1)
        staging = (pltpu.VMEM((2, 136, 1024), bf16), pltpu.SemaphoreType.DMA((2,)))
        kept, sent = piece_sums(y_sum_kernel, summed, staging)
        pieces = (kept, other_zlo(sent))
        half = halves(pieces)
        mine = from_ring(half, Z)
        lefts = from_ring(half, "y")
        rights = mine + [other_core(piece) for piece in mine]
        *parts, right = square_pieces(lefts, rights)
        factor = factor_of(right)
        parts = along_ring(parts, "x")
        near, away = mixed(parts)
        other = other_zhi(away)
        if n == 0:
            square = paired(near, other)
            square = from_ring(square, "x")
        else:
            square = from_ring(near, "x")
            square += from_ring(other, "x")
        parts = cube_pieces(square, factor)
        parts = along_ring(parts, "y")
        parts = cut(parts)
        parts = lax.all_to_all(parts, "x", 0, 0, tiled=True)
        results.append(assembled(parts))
    return tuple(results)


def solution(mesh):
    split = Mesh(mesh.devices.reshape(2, 4, 2, 4, 2), NAMES)
    placed = P(TOK, BLK)
    return jax.shard_map(
        body,
        mesh=split,
        in_specs=(placed, placed),
        out_specs=(P(NAMES, None), P(NAMES, None)),
        check_vma=False,
    )
```

```python
import functools

import jax
import jax.numpy as jnp
from jax import lax
from jax.experimental import pallas as pl
from jax.experimental.pallas import tpu as pltpu
from jax.sharding import Mesh, PartitionSpec as P


D = 4096
TOKENS = 8192
damping = 0.3
epsilon = 1e-06
divisor = 2.0

CENTER = 2.0 / 3.0
P0 = 4.0 - 6.0 * CENTER + 4.0 * CENTER**2 - CENTER**3

NAMES = ("zlo", "y", "core", "x", "zhi")
TOK = ("zlo", "y", "core")
BLK = ("x", "zhi")
Z = ("zlo", "zhi")
STEPS = (1, 2, -1)
f32 = jnp.float32
bf16 = jnp.bfloat16
WHOLE = pl.BlockSpec(memory_space=pltpu.VMEM)
ANYWHERE = pl.BlockSpec(memory_space=pl.ANY)


def shifted_by(value, axis, step):
    place = (lambda z: (z % 2) * 2 + z // 2) if axis == Z else (lambda i: i)
    return lax.ppermute(value, axis, [(place(i), place((i + step) % 4)) for i in range(4)])


def from_ring(value, axis):
    return [value] + [shifted_by(value, axis, step) for step in STEPS]


def along_ring(pieces, axis):
    return [pieces[0]] + [shifted_by(pieces[k], axis, k) for k in range(1, 4)]


def other_core(value):
    return lax.ppermute(value, "core", [(0, 1), (1, 0)])


def other_zlo(value):
    return lax.ppermute(value, "zlo", [(0, 1), (1, 0)])


def other_zhi(value):
    return lax.ppermute(value, "zhi", [(0, 1), (1, 0)])


def position():
    return [lax.axis_index(a) for a in ("x", "y", "core", "zlo", "zhi")]


def call(kernel, outs, operands, specs, scratch=(), flops=0, moved=0, to=WHOLE):
    return pl.pallas_call(
        kernel,
        out_shape=outs,
        in_specs=specs,
        out_specs=jax.tree.map(lambda _: to, outs),
        scratch_shapes=list(scratch),
        compiler_params=pltpu.CompilerParams(vmem_limit_bytes=12 * 1024 * 1024),
        cost_estimate=pl.CostEstimate(flops=flops, bytes_accessed=moved, transcendentals=0),
    )(*operands)


def three_parts(value):
    high = value.astype(bf16).astype(f32)
    rest = value - high
    middle = rest.astype(bf16).astype(f32)
    return high, middle, rest - middle


def sum_rows(of_cols, of_rows):
    row = lax.broadcasted_iota(jnp.int32, (8, 1024), 0)
    of_rows = jnp.concatenate([of_rows, jnp.zeros((1, 896), f32)], axis=1)
    packed = jnp.zeros((8, 1024), f32)
    for k, part in enumerate((*three_parts(of_cols), *three_parts(of_rows))):
        packed = jnp.where(row == k, part, packed)
    return packed.astype(bf16)


def gram_kernel(keep, apart, *refs):
    shards, own, other = refs[:8], refs[8], refs[9]
    received = refs[10] if keep else None
    outs = refs[10 + keep : -5]
    b, a, added, staged, sems = refs[-5:]
    x, y, core, _, zhi = position()
    which = core if keep else 1 - core
    copies = [
        pltpu.make_async_copy(own, a.at[zhi], sems.at[4]),
        pltpu.make_async_copy(other, a.at[1 - zhi], sems.at[5]),
    ]
    stores = []
    for copy in copies:
        copy.start()
    for k, step in enumerate((0, 1, -1, 2)):
        for part in range(2):

            @pl.when(which == part)
            def _():
                pltpu.make_async_copy(shards[2 * k + part], b.at[k], sems.at[k]).start()

        if keep:
            source = lax.rem(x - step + 4, 4)
            pltpu.make_async_copy(received.at[source], added.at[k], sems.at[10 + k]).start()
    for copy in copies:
        copy.wait()
    of_cols = jnp.concatenate(
        [jnp.sum(jnp.square(a[h].astype(f32)), axis=0, keepdims=True) for h in range(2)], axis=1
    )

    def one_shard(k, carry):
        source = lax.rem(x - jnp.where(k == 2, 3, jnp.where(k == 3, 2, k)) + 4, 4)
        pltpu.make_async_copy(shards[0], b.at[k], sems.at[k]).wait()
        if keep:
            pltpu.make_async_copy(received.at[source], added.at[k], sems.at[10 + k]).wait()
        for half in range(2):
            cols = slice(half * 512, (half + 1) * 512)
            piece = jnp.dot(b[k], a[half], preferred_element_type=f32).astype(bf16)
            for part in range(2):
                value = piece[part * 128 : (part + 1) * 128]
                if keep:
                    value = value.astype(f32) + added[k, part, :128, cols].astype(f32)
                staged[source, part, :128, cols] = value.astype(bf16)
        squares = jnp.square(b[k].astype(f32))
        squares = sum(squares[:, q * 128 : (q + 1) * 128] for q in range(4))
        for part in range(2):
            of_rows = jnp.sum(squares[part * 128 : (part + 1) * 128].T, axis=0, keepdims=True)
            cols = of_cols
            if keep:
                more = added[k, part, 128:136].astype(f32)
                cols = cols + more[0:1] + more[1:2] + more[2:3]
                of_rows = of_rows + (more[3:4] + more[4:5] + more[5:6])[:, :128]
            staged[source, part, 128:136] = sum_rows(cols, of_rows)
        if not apart:
            pltpu.make_async_copy(staged.at[source], outs[0].at[source], sems.at[6 + k]).start()
        return carry

    lax.fori_loop(0, 4, one_shard, 0)
    if not apart:
        for k in range(4):
            stores.append(pltpu.make_async_copy(staged.at[k], outs[0].at[k], sems.at[6 + k]))
    if apart:
        for k, out in enumerate(outs):
            to_y = lax.rem(y + k // 2, 4)
            piece = staged.at[k % 2 * 2 + lax.div(to_y, 2), lax.rem(to_y, 2)]
            stores.append(pltpu.make_async_copy(piece, out, sems.at[14 + k]))
            stores[-1].start()
    for copy in stores:
        copy.wait()


def gram_half(keep, apart, shards, own, other, received=()):
    shape = (4, 2, 136, 1024)
    if apart:
        out = (jax.ShapeDtypeStruct((136, 1024), bf16),) * 8
    else:
        out = jax.ShapeDtypeStruct(shape, bf16)
    return call(
        functools.partial(gram_kernel, keep, apart),
        out,
        (*shards, own, other, *received),
        [ANYWHERE] * (10 + keep),
        scratch=[
            pltpu.VMEM((4, 256, 512), bf16),
            pltpu.VMEM((2, 512, 512), bf16),
            pltpu.VMEM(shape if keep else (8, 128), bf16),
            pltpu.VMEM(shape, bf16),
            pltpu.SemaphoreType.DMA((22,)),
        ],
        to=ANYWHERE,
        flops=512 * 1024 * 2048,
        moved=7 << 20,
    )


def turn_kernel(data, top, bottom):
    for k, out in enumerate((top, bottom)):
        out[...] = data[:, k * 256 : (k + 1) * 256].T


def turned(data):
    out = jax.ShapeDtypeStruct((256, 512), bf16)
    return call(turn_kernel, (out, out), (data,), [WHOLE], flops=512 * 512, moved=1 << 20)


def add_up(refs, out):
    def some_rows(k, carry):
        rows = pl.ds(pl.multiple_of(k * 32, 32), 32)
        total = refs[0][rows].astype(f32)
        for ref in refs[1:]:
            total += ref[rows].astype(f32)
        out[rows] = total.astype(bf16)
        return carry

    lax.fori_loop(0, 4, some_rows, 0)
    sums = refs[0][128:136].astype(f32)
    for ref in refs[1:]:
        sums += ref[128:136].astype(f32)
    of_cols = sums[0:1] + sums[1:2] + sums[2:3]
    of_rows = (sums[3:4] + sums[4:5] + sums[5:6])[:, :128]
    out[128:136] = sum_rows(of_cols, of_rows)


def relay_kernel(*refs):
    for k, out in enumerate(refs[4:6]):
        add_up(refs[2 * k : 2 * k + 2], out)


def y_sum_kernel(*refs):
    keep, send, staged, sems = refs[6:]
    zlo = lax.axis_index("zlo")
    for k in range(2):
        add_up(refs[3 * k : 3 * k + 3], staged.at[k])
    copies = [
        pltpu.make_async_copy(staged.at[zlo], keep, sems.at[0]),
        pltpu.make_async_copy(staged.at[1 - zlo], send, sems.at[1]),
    ]
    for copy in copies:
        copy.start()
    for copy in copies:
        copy.wait()


def piece_sums(kernel, pieces, scratch=()):
    out = jax.ShapeDtypeStruct((136, 1024), bf16)
    return call(
        kernel,
        (out, out),
        (*pieces,),
        [WHOLE] * len(pieces),
        scratch=scratch,
        to=ANYWHERE if scratch else WHOLE,
        flops=8 * 136 * 1024,
        moved=2 << 20,
    )


def half_kernel(*refs):
    pieces, half, scale = refs[:-2], refs[-2], refs[-1]
    x, y, core, zlo, zhi = position()
    block = zlo * 16 + lax.div(y, 2) * 8 + zhi * 4 + core * 2 + lax.rem(y, 2)
    sums = pieces[0][128:136].astype(f32)
    for ref in pieces[1:]:
        sums += ref[128:136].astype(f32)
    by_col = lax.rsqrt((sums[0:1] + sums[1:2] + sums[2:3]) / TOKENS + epsilon)
    by_row = lax.rsqrt((sums[3:4] + sums[4:5] + sums[5:6])[:, :128] / TOKENS + epsilon)
    by_row = (jnp.broadcast_to(by_row, (128, 128)) / (TOKENS * divisor)).T
    scale[...] = by_row

    def some_rows(k, carry):
        rows = pl.ds(pl.multiple_of(k * 32, 32), 32)
        row = lax.broadcasted_iota(jnp.int32, (32, 1024), 0) + k * 32
        col = lax.broadcasted_iota(jnp.int32, (32, 1024), 1)
        diagonal = row + (block * 128 - x * 1024) == col
        gram = pieces[0][rows].astype(f32)
        for ref in pieces[1:]:
            gram += ref[rows].astype(f32)
        value = gram * scale[rows, :1] * by_col
        value += jnp.where(diagonal, damping / divisor - CENTER, 0.0)
        half[rows] = value.astype(bf16)
        return carry

    lax.fori_loop(0, 4, some_rows, 0)


def halves(pieces):
    return call(
        half_kernel,
        jax.ShapeDtypeStruct((128, 1024), bf16),
        (*pieces,),
        [WHOLE] * len(pieces),
        scratch=[pltpu.VMEM((128, 128), f32)],
        flops=20 * 128 * 1024,
        moved=3 << 20,
    )


def square_kernel(*refs):
    lefts, rights, outs, right = refs[:4], refs[4:12], refs[12:16], refs[16]
    left, sems = refs[17:]
    x, y, core, zlo, zhi = position()
    z = zhi * 2 + zlo
    copies = []
    for k, (ref, step) in enumerate(zip(lefts, (0, *STEPS))):
        slot = lax.rem(y - step - x + 8, 4)
        copies.append(
            pltpu.make_async_copy(
                ref, left.at[pl.ds(pl.multiple_of(slot * 128, 128), 128)], sems.at[k]
            )
        )
    for k, ref in enumerate(rights):
        slot = (k // 4) * 4 + lax.rem(z - (0, *STEPS)[k % 4] + 4, 4)
        copies.append(
            pltpu.make_async_copy(
                ref, right.at[pl.ds(pl.multiple_of(slot * 128, 128), 128)], sems.at[4 + k]
            )
        )
    for copy in copies:
        copy.start()
    for copy in copies:
        copy.wait()
    meets = (lax.rem(x, 2) == lax.div(y, 2)).astype(f32)

    def some_columns(n, carry):
        rows = pl.ds(pl.multiple_of(n * 256, 256), 256)
        product = lax.dot_general(
            left[...], right[rows], (((1,), (1,)), ((), ())), preferred_element_type=f32
        )
        of_core = jnp.where(n < 2, core, 1 - core)
        for of_zlo in range(2):
            scale = meets * (lax.div(x, 2) == of_zlo).astype(f32)
            at = lax.rem(n, 2) * 512 + of_core * 256 + lax.rem(y, 2) * 128
            term = left[:, pl.ds(pl.multiple_of(at, 128), 128)].astype(f32)
            value = product[:, of_zlo * 128 : (of_zlo + 1) * 128] - scale * term
            value = value.astype(bf16)
            cols = pl.ds(pl.multiple_of(n * 256 + of_zlo * 128, 128), 128)
            for k, out in enumerate(outs):
                out[:, cols] = value[k * 128 : (k + 1) * 128]
        return carry

    lax.fori_loop(0, 4, some_columns, 0)


def square_pieces(lefts, rights):
    out = jax.ShapeDtypeStruct((128, 1024), bf16)
    return call(
        square_kernel,
        (out,) * 4 + (jax.ShapeDtypeStruct((1024, 1024), bf16),),
        (*lefts, *rights),
        [ANYWHERE] * 12,
        scratch=[
            pltpu.VMEM((512, 1024), bf16),
            pltpu.SemaphoreType.DMA((12,)),
        ],
        flops=2 * 512 * 1024 * 1024,
        moved=4 << 20,
    )


def factor_kernel(right, out, staged, sems):
    x, y, core, _, _ = position()
    row = lax.broadcasted_iota(jnp.int32, (128, 1024), 0)
    col = lax.broadcasted_iota(jnp.int32, (128, 1024), 1)

    def one_block(k, carry):
        of_core = jnp.where(k < 4, core, 1 - core)
        of_z = lax.rem(k, 4)
        block = lax.rem(k, 2) * 16 + lax.div(y, 2) * 8 + lax.div(of_z, 2) * 4
        block += of_core * 2 + lax.rem(y, 2)
        diagonal = row + (block * 128 - x * 1024) == col
        rows = pl.ds(pl.multiple_of(k * 128, 128), 128)
        staged[rows] = (jnp.where(diagonal, 1.0, 0.0) - right[rows].astype(f32)).astype(bf16)
        pltpu.make_async_copy(staged.at[rows], out.at[rows], sems.at[k]).start()
        return carry

    lax.fori_loop(0, 8, one_block, 0)
    for k in range(8):
        rows = pl.ds(k * 128, 128)
        pltpu.make_async_copy(staged.at[rows], out.at[rows], sems.at[k]).wait()


def factor_of(right):
    return call(
        factor_kernel,
        pltpu.HBM((1024, 1024), bf16),
        (right,),
        [WHOLE],
        scratch=[pltpu.VMEM((1024, 1024), bf16), pltpu.SemaphoreType.DMA((8,))],
        flops=4 * 1024 * 1024,
        moved=4 << 20,
        to=ANYWHERE,
    )


def mix_kernel(*refs):
    pieces, outs = refs[:4], refs[4:]
    x, y, _, zlo, zhi = position()
    row = lax.broadcasted_iota(jnp.int32, (32, 1024), 0)
    col = lax.broadcasted_iota(jnp.int32, (32, 1024), 1)
    first = jnp.where(x == y, (zhi * 2 + zlo) * 128, 4096)
    for away, out in enumerate(outs):
        f5 = 1 - zhi if away else zhi
        for f6 in range(2):
            at = f6 * 64 + f5 * 32
            rows = pl.ds(pl.multiple_of(at, 32), 32)
            total = pieces[0][rows].astype(f32)
            for ref in pieces[1:]:
                total += ref[rows].astype(f32)
            total += jnp.where(row + (first + at) == col, 1.0, 0.0)
            out[f6 * 32 : (f6 + 1) * 32] = total.astype(bf16)


def mixed(pieces):
    small = jax.ShapeDtypeStruct((64, 1024), bf16)
    return call(
        mix_kernel, (small, small), (*pieces,), [WHOLE] * 4, flops=8 * 128 * 1024, moved=2 << 20
    )


def pair_kernel(own, other, out):
    zhi = lax.axis_index("zhi")
    out[pl.ds(pl.multiple_of(zhi * 64, 64), 64)] = own[...]
    out[pl.ds(pl.multiple_of((1 - zhi) * 64, 64), 64)] = other[...]


def paired(own, other):
    return call(
        pair_kernel,
        jax.ShapeDtypeStruct((128, 1024), bf16),
        (own, other),
        [WHOLE] * 2,
        flops=128 * 1024,
        moved=1 << 19,
    )


def cube_kernel(*refs):
    squares_in, factor_in, outs = refs[:-9], refs[-9], refs[-8:-4]
    factor, total, squares, sems = refs[-4:]
    x, y, _, _, zhi = position()
    copies = [pltpu.make_async_copy(factor_in, factor, sems.at[8])]
    for k, ref in enumerate(squares_in):
        at = lax.rem(x - (0, *STEPS)[k % 4] + 4, 4) * 128
        if len(squares_in) == 8:
            at += 64 * (zhi if k < 4 else 1 - zhi)
        at = pl.ds(pl.multiple_of(at, 64), ref.shape[0])
        copies.append(pltpu.make_async_copy(ref, squares.at[at], sems.at[k]))
    for copy in copies:
        copy.start()
    for copy in copies:
        copy.wait()

    def some_columns(n, carry):
        cols = pl.ds(pl.multiple_of(n * 256, 256), 256)
        total[:, cols] = jnp.dot(squares[...], factor[:, cols], preferred_element_type=f32)
        return carry

    lax.fori_loop(0, 4, some_columns, 0)
    for k, out in enumerate(outs):
        to_y = lax.rem(y + k, 4)
        for f7 in range(2):
            at = ((lax.div(to_y, 2) * 2 + f7) * 2 + lax.rem(to_y, 2)) * 64
            out[f7 * 64 : (f7 + 1) * 64] = total[pl.ds(pl.multiple_of(at, 64), 64)].astype(bf16)


def cube_pieces(squares, factor):
    out = jax.ShapeDtypeStruct((128, 1024), bf16)
    return call(
        cube_kernel,
        (out,) * 4,
        (*squares, factor),
        [ANYWHERE] * (len(squares) + 1),
        scratch=[
            pltpu.VMEM((1024, 1024), bf16),
            pltpu.VMEM((512, 1024), f32),
            pltpu.VMEM((512, 1024), bf16),
            pltpu.SemaphoreType.DMA((9,)),
        ],
        flops=2 * 512 * 1024 * 1024,
        moved=4 << 20,
    )


def cut_kernel(*refs):
    pieces, outs = refs[:4], refs[4:]
    x = lax.axis_index("x")
    for k, out in enumerate(outs):
        rows = pl.ds(pl.multiple_of(lax.rem(x + k, 4) * 32, 32), 32)
        total = pieces[0][rows].astype(f32)
        for ref in pieces[1:]:
            total += ref[rows].astype(f32)
        out[...] = total.astype(bf16)


def cut(pieces):
    out = jax.ShapeDtypeStruct((32, 1024), bf16)
    return call(
        cut_kernel, (out,) * 4, (*pieces,), [WHOLE] * 4, flops=4 * 128 * 1024, moved=2 << 20
    )


def out_kernel(*refs):
    pieces, out = refs[:4], refs[4]
    x, y, core, zlo, zhi = position()
    first = (((zlo * 4 + y) * 2 + core) * 8 + x * 2 + zhi) * 32
    row = lax.broadcasted_iota(jnp.int32, (32, 1024), 0)
    col = lax.broadcasted_iota(jnp.int32, (32, 1024), 1)
    for k, ref in enumerate(pieces):
        source = lax.rem(x - k + 4, 4)
        diagonal = row + (first - source * 1024) == col
        out[:, pl.ds(pl.multiple_of(source * 1024, 1024), 1024)] = ref[...].astype(
            f32
        ) + jnp.where(diagonal, P0 - 1.0, 0.0)


def assembled(pieces):
    return call(
        out_kernel,
        jax.ShapeDtypeStruct((32, D), f32),
        (*pieces,),
        [WHOLE] * 4,
        flops=2 * 32 * D,
        moved=1 << 20,
    )


def body(activations, out_grads):
    zlo, y, core = (lax.axis_index(a) for a in TOK)
    x, zhi = (lax.axis_index(a) for a in BLK)
    both = (activations, out_grads)

    results = []
    for n, data in enumerate(both):
        own = turned(data)
        left_top = shifted_by(own[0], "x", 1)
        right_bottom = shifted_by(own[1], "x", -1)
        left_bottom = shifted_by(own[1], "x", 1)
        right_top = shifted_by(own[0], "x", -1)
        away = other_zhi(data)
        far_top = shifted_by(left_top, "x", 1)
        far_bottom = shifted_by(right_bottom, "x", -1)
        shards = (*own, left_top, left_bottom, right_top, right_bottom, far_top, far_bottom)
        sent = gram_half(False, False, shards, data, away)
        received = other_core(sent)
        pieces = gram_half(True, True, shards, data, away, (received,))
        here, after, far, before = (pieces[2 * k : 2 * k + 2] for k in range(4))
        far_up = shifted_by(far[0], "y", 1)
        far_down = shifted_by(far[1], "y", -1)
        up_1 = shifted_by(after[1], "y", 1)
        down_0 = shifted_by(before[0], "y", -1)
        summed = (after[0], far_up, before[1], far_down)
        up_0, down_1 = piece_sums(relay_kernel, summed)
        up_0 = shifted_by(up_0, "y", 1)
        down_1 = shifted_by(down_1, "y", -1)
        summed = (here[0], up_0, down_0, here[1], up_1, down_1)
        staging = (pltpu.VMEM((2, 136, 1024), bf16), pltpu.SemaphoreType.DMA((2,)))
        kept, sent = piece_sums(y_sum_kernel, summed, staging)
        pieces = (kept, other_zlo(sent))
        half = halves(pieces)
        mine = from_ring(half, Z)
        lefts = from_ring(half, "y")
        rights = mine + [other_core(piece) for piece in mine]
        *parts, right = square_pieces(lefts, rights)
        factor = factor_of(right)
        parts = along_ring(parts, "x")
        near, away = mixed(parts)
        other = other_zhi(away)
        if n == 0:
            square = paired(near, other)
            square = from_ring(square, "x")
        else:
            square = from_ring(near, "x")
            square += from_ring(other, "x")
        parts = cube_pieces(square, factor)
        parts = along_ring(parts, "y")
        parts = cut(parts)
        parts = along_ring(parts, "x")
        results.append(assembled(parts))
    return tuple(results)


def solution(mesh):
    split = Mesh(mesh.devices.reshape(2, 4, 2, 4, 2), NAMES)
    placed = P(TOK, BLK)
    return jax.shard_map(
        body,
        mesh=split,
        in_specs=(placed, placed),
        out_specs=(P(NAMES, None), P(NAMES, None)),
        check_vma=False,
    )
```

```python
import functools

import jax
import jax.numpy as jnp
from jax import lax
from jax.experimental import pallas as pl
from jax.experimental.pallas import tpu as pltpu
from jax.sharding import Mesh, PartitionSpec as P


D = 4096
TOKENS = 8192
damping = 0.3
epsilon = 1e-06
divisor = 2.0

CENTER = 2.0 / 3.0
P0 = 4.0 - 6.0 * CENTER + 4.0 * CENTER**2 - CENTER**3

NAMES = ("zlo", "y", "core", "x", "zhi")
TOK = ("zlo", "y", "core")
BLK = ("x", "zhi")
Z = ("zlo", "zhi")
STEPS = (1, -1, 2)
f32 = jnp.float32
bf16 = jnp.bfloat16
WHOLE = pl.BlockSpec(memory_space=pltpu.VMEM)
ANYWHERE = pl.BlockSpec(memory_space=pl.ANY)


def shifted_by(value, axis, step):
    place = (lambda z: (z % 2) * 2 + z // 2) if axis == Z else (lambda i: i)
    return lax.ppermute(value, axis, [(place(i), place((i + step) % 4)) for i in range(4)])


def from_ring(value, axis):
    return [value] + [shifted_by(value, axis, step) for step in STEPS]


def along_ring(pieces, axis):
    return [pieces[0]] + [shifted_by(pieces[k], axis, k) for k in range(1, 4)]


def other_core(value):
    return lax.ppermute(value, "core", [(0, 1), (1, 0)])


def other_zlo(value):
    return lax.ppermute(value, "zlo", [(0, 1), (1, 0)])


def other_zhi(value):
    return lax.ppermute(value, "zhi", [(0, 1), (1, 0)])


def position():
    return [lax.axis_index(a) for a in ("x", "y", "core", "zlo", "zhi")]


def call(kernel, outs, operands, specs, scratch=(), flops=0, moved=0, to=WHOLE):
    return pl.pallas_call(
        kernel,
        out_shape=outs,
        in_specs=specs,
        out_specs=jax.tree.map(lambda _: to, outs),
        scratch_shapes=list(scratch),
        compiler_params=pltpu.CompilerParams(vmem_limit_bytes=12 * 1024 * 1024),
        cost_estimate=pl.CostEstimate(flops=flops, bytes_accessed=moved, transcendentals=0),
    )(*operands)


def three_parts(value):
    high = value.astype(bf16).astype(f32)
    rest = value - high
    middle = rest.astype(bf16).astype(f32)
    return high, middle, rest - middle


def sum_rows(of_cols, of_rows):
    row = lax.broadcasted_iota(jnp.int32, (8, 1024), 0)
    of_rows = jnp.concatenate([of_rows, jnp.zeros((1, 896), f32)], axis=1)
    packed = jnp.zeros((8, 1024), f32)
    for k, part in enumerate((*three_parts(of_cols), *three_parts(of_rows))):
        packed = jnp.where(row == k, part, packed)
    return packed.astype(bf16)


def gram_kernel(keep, apart, *refs):
    shards, own, other = refs[:8], refs[8], refs[9]
    received = refs[10] if keep else None
    outs = refs[10 + keep : -5]
    b, a, added, staged, sems = refs[-5:]
    x, y, core, _, zhi = position()
    which = core if keep else 1 - core
    copies = [
        pltpu.make_async_copy(own, a.at[zhi], sems.at[4]),
        pltpu.make_async_copy(other, a.at[1 - zhi], sems.at[5]),
    ]
    stores = []
    for copy in copies:
        copy.start()
    for k, step in enumerate((0, *STEPS)):
        for part in range(2):

            @pl.when(which == part)
            def _():
                pltpu.make_async_copy(shards[2 * k + part], b.at[k], sems.at[k]).start()

        if keep:
            source = lax.rem(x - step + 4, 4)
            pltpu.make_async_copy(received.at[source], added.at[k], sems.at[10 + k]).start()
    for copy in copies:
        copy.wait()
    of_cols = jnp.concatenate(
        [jnp.sum(jnp.square(a[h].astype(f32)), axis=0, keepdims=True) for h in range(2)], axis=1
    )

    def one_shard(k, carry):
        source = lax.rem(x - jnp.where(k == 2, 3, jnp.where(k == 3, 2, k)) + 4, 4)
        pltpu.make_async_copy(shards[0], b.at[k], sems.at[k]).wait()
        if keep:
            pltpu.make_async_copy(received.at[source], added.at[k], sems.at[10 + k]).wait()
        for half in range(2):
            cols = slice(half * 512, (half + 1) * 512)
            piece = jnp.dot(b[k], a[half], preferred_element_type=f32).astype(bf16)
            for part in range(2):
                value = piece[part * 128 : (part + 1) * 128]
                if keep:
                    value = value.astype(f32) + added[k, part, :128, cols].astype(f32)
                staged[source, part, :128, cols] = value.astype(bf16)
        squares = jnp.square(b[k].astype(f32))
        squares = sum(squares[:, q * 128 : (q + 1) * 128] for q in range(4))
        for part in range(2):
            of_rows = jnp.sum(squares[part * 128 : (part + 1) * 128].T, axis=0, keepdims=True)
            cols = of_cols
            if keep:
                more = added[k, part, 128:136].astype(f32)
                cols = cols + more[0:1] + more[1:2] + more[2:3]
                of_rows = of_rows + (more[3:4] + more[4:5] + more[5:6])[:, :128]
            staged[source, part, 128:136] = sum_rows(cols, of_rows)
        if not apart:
            pltpu.make_async_copy(staged.at[source], outs[0].at[source], sems.at[6 + k]).start()
        return carry

    lax.fori_loop(0, 4, one_shard, 0)
    if not apart:
        for k in range(4):
            stores.append(pltpu.make_async_copy(staged.at[k], outs[0].at[k], sems.at[6 + k]))
    if apart:
        for k, out in enumerate(outs):
            to_y = lax.rem(y + k // 2, 4)
            piece = staged.at[k % 2 * 2 + lax.div(to_y, 2), lax.rem(to_y, 2)]
            stores.append(pltpu.make_async_copy(piece, out, sems.at[14 + k]))
            stores[-1].start()
    for copy in stores:
        copy.wait()


def gram_half(keep, apart, shards, own, other, received=()):
    shape = (4, 2, 136, 1024)
    if apart:
        out = (jax.ShapeDtypeStruct((136, 1024), bf16),) * 8
    else:
        out = jax.ShapeDtypeStruct(shape, bf16)
    return call(
        functools.partial(gram_kernel, keep, apart),
        out,
        (*shards, own, other, *received),
        [ANYWHERE] * (10 + keep),
        scratch=[
            pltpu.VMEM((4, 256, 512), bf16),
            pltpu.VMEM((2, 512, 512), bf16),
            pltpu.VMEM(shape if keep else (8, 128), bf16),
            pltpu.VMEM(shape, bf16),
            pltpu.SemaphoreType.DMA((22,)),
        ],
        to=ANYWHERE,
        flops=512 * 1024 * 2048,
        moved=7 << 20,
    )


def turn_kernel(data, top, bottom):
    for k, out in enumerate((top, bottom)):
        out[...] = data[:, k * 256 : (k + 1) * 256].T


def turned(data):
    out = jax.ShapeDtypeStruct((256, 512), bf16)
    return call(turn_kernel, (out, out), (data,), [WHOLE], flops=512 * 512, moved=1 << 20)


def add_up(refs, out):
    def some_rows(k, carry):
        rows = pl.ds(pl.multiple_of(k * 32, 32), 32)
        total = refs[0][rows].astype(f32)
        for ref in refs[1:]:
            total += ref[rows].astype(f32)
        out[rows] = total.astype(bf16)
        return carry

    lax.fori_loop(0, 4, some_rows, 0)
    sums = refs[0][128:136].astype(f32)
    for ref in refs[1:]:
        sums += ref[128:136].astype(f32)
    of_cols = sums[0:1] + sums[1:2] + sums[2:3]
    of_rows = (sums[3:4] + sums[4:5] + sums[5:6])[:, :128]
    out[128:136] = sum_rows(of_cols, of_rows)


def relay_kernel(*refs):
    for k, out in enumerate(refs[4:6]):
        add_up(refs[2 * k : 2 * k + 2], out)


def y_sum_kernel(*refs):
    keep, send, staged, sems = refs[6:]
    zlo = lax.axis_index("zlo")
    for k in range(2):
        add_up(refs[3 * k : 3 * k + 3], staged.at[k])
    copies = [
        pltpu.make_async_copy(staged.at[zlo], keep, sems.at[0]),
        pltpu.make_async_copy(staged.at[1 - zlo], send, sems.at[1]),
    ]
    for copy in copies:
        copy.start()
    for copy in copies:
        copy.wait()


def piece_sums(kernel, pieces, scratch=()):
    out = jax.ShapeDtypeStruct((136, 1024), bf16)
    return call(
        kernel,
        (out, out),
        (*pieces,),
        [WHOLE] * len(pieces),
        scratch=scratch,
        to=ANYWHERE if scratch else WHOLE,
        flops=8 * 136 * 1024,
        moved=2 << 20,
    )


def half_kernel(*refs):
    pieces, half, scale = refs[:-2], refs[-2], refs[-1]
    x, y, core, zlo, zhi = position()
    block = zlo * 16 + lax.div(y, 2) * 8 + zhi * 4 + core * 2 + lax.rem(y, 2)
    sums = pieces[0][128:136].astype(f32)
    for ref in pieces[1:]:
        sums += ref[128:136].astype(f32)
    by_col = lax.rsqrt((sums[0:1] + sums[1:2] + sums[2:3]) / TOKENS + epsilon)
    by_row = lax.rsqrt((sums[3:4] + sums[4:5] + sums[5:6])[:, :128] / TOKENS + epsilon)
    by_row = (jnp.broadcast_to(by_row, (128, 128)) / (TOKENS * divisor)).T
    scale[...] = by_row

    def some_rows(k, carry):
        rows = pl.ds(pl.multiple_of(k * 32, 32), 32)
        row = lax.broadcasted_iota(jnp.int32, (32, 1024), 0) + k * 32
        col = lax.broadcasted_iota(jnp.int32, (32, 1024), 1)
        diagonal = row + (block * 128 - x * 1024) == col
        gram = pieces[0][rows].astype(f32)
        for ref in pieces[1:]:
            gram += ref[rows].astype(f32)
        value = gram * scale[rows, :1] * by_col
        value += jnp.where(diagonal, damping / divisor - CENTER, 0.0)
        half[rows] = value.astype(bf16)
        return carry

    lax.fori_loop(0, 4, some_rows, 0)


def halves(pieces):
    return call(
        half_kernel,
        jax.ShapeDtypeStruct((128, 1024), bf16),
        (*pieces,),
        [WHOLE] * len(pieces),
        scratch=[pltpu.VMEM((128, 128), f32)],
        flops=20 * 128 * 1024,
        moved=3 << 20,
    )


def square_kernel(*refs):
    lefts, rights, outs, right = refs[:4], refs[4:12], refs[12:16], refs[16]
    left, sems = refs[17:]
    x, y, core, zlo, zhi = position()
    z = zhi * 2 + zlo
    copies = []
    for k, (ref, step) in enumerate(zip(lefts, (0, *STEPS))):
        slot = lax.rem(y - step - x + 8, 4)
        copies.append(
            pltpu.make_async_copy(
                ref, left.at[pl.ds(pl.multiple_of(slot * 128, 128), 128)], sems.at[k]
            )
        )
    for k, ref in enumerate(rights):
        slot = (k // 4) * 4 + lax.rem(z - (0, *STEPS)[k % 4] + 4, 4)
        copies.append(
            pltpu.make_async_copy(
                ref, right.at[pl.ds(pl.multiple_of(slot * 128, 128), 128)], sems.at[4 + k]
            )
        )
    for copy in copies:
        copy.start()
    for copy in copies:
        copy.wait()
    meets = (lax.rem(x, 2) == lax.div(y, 2)).astype(f32)

    def some_columns(n, carry):
        rows = pl.ds(pl.multiple_of(n * 256, 256), 256)
        product = lax.dot_general(
            left[...], right[rows], (((1,), (1,)), ((), ())), preferred_element_type=f32
        )
        of_core = jnp.where(n < 2, core, 1 - core)
        for of_zlo in range(2):
            scale = meets * (lax.div(x, 2) == of_zlo).astype(f32)
            at = lax.rem(n, 2) * 512 + of_core * 256 + lax.rem(y, 2) * 128
            term = left[:, pl.ds(pl.multiple_of(at, 128), 128)].astype(f32)
            value = product[:, of_zlo * 128 : (of_zlo + 1) * 128] - scale * term
            value = value.astype(bf16)
            cols = pl.ds(pl.multiple_of(n * 256 + of_zlo * 128, 128), 128)
            for k, out in enumerate(outs):
                out[:, cols] = value[k * 128 : (k + 1) * 128]
        return carry

    lax.fori_loop(0, 4, some_columns, 0)


def square_pieces(lefts, rights):
    out = jax.ShapeDtypeStruct((128, 1024), bf16)
    return call(
        square_kernel,
        (out,) * 4 + (jax.ShapeDtypeStruct((1024, 1024), bf16),),
        (*lefts, *rights),
        [ANYWHERE] * 12,
        scratch=[
            pltpu.VMEM((512, 1024), bf16),
            pltpu.SemaphoreType.DMA((12,)),
        ],
        flops=2 * 512 * 1024 * 1024,
        moved=4 << 20,
    )


def factor_kernel(right, out, staged, sems):
    x, y, core, _, _ = position()
    row = lax.broadcasted_iota(jnp.int32, (128, 1024), 0)
    col = lax.broadcasted_iota(jnp.int32, (128, 1024), 1)

    def one_block(k, carry):
        of_core = jnp.where(k < 4, core, 1 - core)
        of_z = lax.rem(k, 4)
        block = lax.rem(k, 2) * 16 + lax.div(y, 2) * 8 + lax.div(of_z, 2) * 4
        block += of_core * 2 + lax.rem(y, 2)
        diagonal = row + (block * 128 - x * 1024) == col
        rows = pl.ds(pl.multiple_of(k * 128, 128), 128)
        staged[rows] = (jnp.where(diagonal, 1.0, 0.0) - right[rows].astype(f32)).astype(bf16)
        pltpu.make_async_copy(staged.at[rows], out.at[rows], sems.at[k]).start()
        return carry

    lax.fori_loop(0, 8, one_block, 0)
    for k in range(8):
        rows = pl.ds(k * 128, 128)
        pltpu.make_async_copy(staged.at[rows], out.at[rows], sems.at[k]).wait()


def factor_of(right):
    return call(
        factor_kernel,
        pltpu.HBM((1024, 1024), bf16),
        (right,),
        [WHOLE],
        scratch=[pltpu.VMEM((1024, 1024), bf16), pltpu.SemaphoreType.DMA((8,))],
        flops=4 * 1024 * 1024,
        moved=4 << 20,
        to=ANYWHERE,
    )


def mix_kernel(*refs):
    pieces, outs = refs[:4], refs[4:]
    x, y, _, zlo, zhi = position()
    row = lax.broadcasted_iota(jnp.int32, (32, 1024), 0)
    col = lax.broadcasted_iota(jnp.int32, (32, 1024), 1)
    first = jnp.where(x == y, (zhi * 2 + zlo) * 128, 4096)

    def some_rows(f6, carry):
        for away, out in enumerate(outs):
            at = f6 * 64 + (1 - zhi if away else zhi) * 32
            rows = pl.ds(pl.multiple_of(at, 32), 32)
            total = pieces[0][rows].astype(f32)
            for ref in pieces[1:]:
                total += ref[rows].astype(f32)
            total += jnp.where(row + (first + at) == col, 1.0, 0.0)
            out[pl.ds(pl.multiple_of(f6 * 32, 32), 32)] = total.astype(bf16)
        return carry

    lax.fori_loop(0, 2, some_rows, 0)


def mixed(pieces):
    small = jax.ShapeDtypeStruct((64, 1024), bf16)
    return call(
        mix_kernel, (small, small), (*pieces,), [WHOLE] * 4, flops=8 * 128 * 1024, moved=2 << 20
    )


def cube_kernel(*refs):
    squares_in, factor_in, outs = refs[:-9], refs[-9], refs[-8:-4]
    factor, total, squares, sems = refs[-4:]
    x, y, _, _, zhi = position()
    copies = [pltpu.make_async_copy(factor_in, factor, sems.at[8])]
    for k, ref in enumerate(squares_in):
        at = lax.rem(x - (0, *STEPS)[k % 4] + 4, 4) * 128
        if len(squares_in) == 8:
            at += 64 * (zhi if k < 4 else 1 - zhi)
        at = pl.ds(pl.multiple_of(at, 64), ref.shape[0])
        copies.append(pltpu.make_async_copy(ref, squares.at[at], sems.at[k]))
    for copy in copies:
        copy.start()
    for copy in copies:
        copy.wait()

    def some_columns(n, carry):
        cols = pl.ds(pl.multiple_of(n * 256, 256), 256)
        total[:, cols] = jnp.dot(squares[...], factor[:, cols], preferred_element_type=f32)
        return carry

    lax.fori_loop(0, 4, some_columns, 0)

    def some_rows(n, carry):
        f7, part = lax.div(n, 2), lax.rem(n, 2) * 32
        to = pl.ds(pl.multiple_of(n * 32, 32), 32)
        for k, out in enumerate(outs):
            to_y = lax.rem(y + k, 4)
            at = ((lax.div(to_y, 2) * 2 + f7) * 2 + lax.rem(to_y, 2)) * 64 + part
            out[to] = total[pl.ds(pl.multiple_of(at, 32), 32)].astype(bf16)
        return carry

    lax.fori_loop(0, 4, some_rows, 0)


def cube_pieces(squares, factor):
    out = jax.ShapeDtypeStruct((128, 1024), bf16)
    return call(
        cube_kernel,
        (out,) * 4,
        (*squares, factor),
        [ANYWHERE] * (len(squares) + 1),
        scratch=[
            pltpu.VMEM((1024, 1024), bf16),
            pltpu.VMEM((512, 1024), f32),
            pltpu.VMEM((512, 1024), bf16),
            pltpu.SemaphoreType.DMA((9,)),
        ],
        flops=2 * 512 * 1024 * 1024,
        moved=4 << 20,
    )


def cut_kernel(*refs):
    pieces, outs = refs[:4], refs[4:]
    x = lax.axis_index("x")
    for k, out in enumerate(outs):
        rows = pl.ds(pl.multiple_of(lax.rem(x + k, 4) * 32, 32), 32)
        total = pieces[0][rows].astype(f32)
        for ref in pieces[1:]:
            total += ref[rows].astype(f32)
        out[...] = total.astype(bf16)


def cut(pieces):
    out = jax.ShapeDtypeStruct((32, 1024), bf16)
    return call(
        cut_kernel, (out,) * 4, (*pieces,), [WHOLE] * 4, flops=4 * 128 * 1024, moved=2 << 20
    )


def out_kernel(*refs):
    pieces, out = refs[:4], refs[4]
    x, y, core, zlo, zhi = position()
    first = (((zlo * 4 + y) * 2 + core) * 8 + x * 2 + zhi) * 32
    row = lax.broadcasted_iota(jnp.int32, (32, 1024), 0)
    col = lax.broadcasted_iota(jnp.int32, (32, 1024), 1)
    for k, ref in enumerate(pieces):
        source = lax.rem(x - k + 4, 4)
        diagonal = row + (first - source * 1024) == col
        out[:, pl.ds(pl.multiple_of(source * 1024, 1024), 1024)] = ref[...].astype(
            f32
        ) + jnp.where(diagonal, P0 - 1.0, 0.0)


def assembled(pieces):
    return call(
        out_kernel,
        jax.ShapeDtypeStruct((32, D), f32),
        (*pieces,),
        [WHOLE] * 4,
        flops=2 * 32 * D,
        moved=1 << 20,
    )


def body(activations, out_grads):
    zlo, y, core = (lax.axis_index(a) for a in TOK)
    x, zhi = (lax.axis_index(a) for a in BLK)
    both = (activations, out_grads)

    results = []
    for data in both:
        own = turned(data)
        left_top = shifted_by(own[0], "x", 1)
        right_bottom = shifted_by(own[1], "x", -1)
        left_bottom = shifted_by(own[1], "x", 1)
        right_top = shifted_by(own[0], "x", -1)
        away = other_zhi(data)
        far_top = shifted_by(left_top, "x", 1)
        far_bottom = shifted_by(right_bottom, "x", -1)
        shards = (*own, left_top, left_bottom, right_top, right_bottom, far_top, far_bottom)
        sent = gram_half(False, False, shards, data, away)
        received = other_core(sent)
        pieces = gram_half(True, True, shards, data, away, (received,))
        here, after, far, before = (pieces[2 * k : 2 * k + 2] for k in range(4))
        far_up = shifted_by(far[0], "y", 1)
        far_down = shifted_by(far[1], "y", -1)
        up_1 = shifted_by(after[1], "y", 1)
        down_0 = shifted_by(before[0], "y", -1)
        summed = (after[0], far_up, before[1], far_down)
        up_0, down_1 = piece_sums(relay_kernel, summed)
        up_0 = shifted_by(up_0, "y", 1)
        down_1 = shifted_by(down_1, "y", -1)
        summed = (here[0], up_0, down_0, here[1], up_1, down_1)
        staging = (pltpu.VMEM((2, 136, 1024), bf16), pltpu.SemaphoreType.DMA((2,)))
        kept, sent = piece_sums(y_sum_kernel, summed, staging)
        pieces = (kept, other_zlo(sent))
        half = halves(pieces)
        mine = from_ring(half, Z)
        lefts = from_ring(half, "y")
        rights = mine + [other_core(piece) for piece in mine]
        *parts, right = square_pieces(lefts, rights)
        factor = factor_of(right)
        parts = along_ring(parts, "x")
        near, away = mixed(parts)
        other = other_zhi(away)
        square = from_ring(near, "x")
        square += from_ring(other, "x")
        parts = cube_pieces(square, factor)
        parts = along_ring(parts, "y")
        parts = cut(parts)
        parts = along_ring(parts, "x")
        results.append(assembled(parts))
    return tuple(results)


def solution(mesh):
    split = Mesh(mesh.devices.reshape(2, 4, 2, 4, 2), NAMES)
    placed = P(TOK, BLK)
    return jax.shard_map(
        body,
        mesh=split,
        in_specs=(placed, placed),
        out_specs=(P(NAMES, None), P(NAMES, None)),
        check_vma=False,
    )
```
